32 devices in a mesh: dp: 4 (over y, x), fsdp: 8 (over z, core).
Axes of the slice: x: 2, y: 2, z: 4, core: 2. Of those that a mesh axis runs over, the one named last changes fastest.
Arguments:
- tokens: bfloat16 [32, 1024, 768], P(('dp', 'fsdp')), may hold values from -6 to 6
- lengths: int32 [32], P(('dp', 'fsdp')), may hold values from 256 to 1024, as said below
- cells: int32 [32, 1024], P(('dp', 'fsdp')), may hold values 0 or 1
- cotangent: bfloat16 [32, 1024, 768], P(('dp', 'fsdp')), may hold values from -6 to 6
- ln1_gain: bfloat16 [768], P('fsdp'), may hold values from 0.5 to 1.5
- ln1_bias: bfloat16 [768], P('fsdp'), may hold values from -3 to 3
- w_qkv: bfloat16 [768, 2304], P('fsdp'), may hold values from -0.21875 to 0.21875
- b_query: bfloat16 [768], P('fsdp'), may hold values from -6 to 6
- b_value: bfloat16 [768], P('fsdp'), may hold values from -6 to 6
- w_out: bfloat16 [768, 768], P('fsdp'), may hold values from -0.875 to 0.875
- b_out: bfloat16 [768], P('fsdp'), may hold values from -3 to 3
- ln2_gain: bfloat16 [768], P('fsdp'), may hold values from 0.5 to 1.5
- ln2_bias: bfloat16 [768], P('fsdp'), may hold values from -3 to 3
- w_up: bfloat16 [768, 3072], P('fsdp'), may hold values from -0.21875 to 0.21875
- b_up: bfloat16 [3072], P('fsdp'), may hold values from -3 to 3
- w_down: bfloat16 [3072, 768], P('fsdp'), may hold values from -0.109375 to 0.109375
- b_down: bfloat16 [768], P('fsdp'), may hold values from -3 to 3
Outputs:
- output: bfloat16 [32, 1024, 768], P(('dp', 'fsdp'))
- grad_tokens: float32 [32, 1024, 768], P(('dp', 'fsdp'))
- grad_ln1_gain: float32 [768], P('fsdp')
- grad_ln1_bias: float32 [768], P('fsdp')
- grad_w_qkv: float32 [768, 2304], P('fsdp')
- grad_b_query: float32 [768], P('fsdp')
- grad_b_value: float32 [768], P('fsdp')
- grad_w_out: float32 [768, 768], P('fsdp')
- grad_b_out: float32 [768], P('fsdp')
- grad_ln2_gain: float32 [768], P('fsdp')
- grad_ln2_bias: float32 [768], P('fsdp')
- grad_w_up: float32 [768, 3072], P('fsdp')
- grad_b_up: float32 [3072], P('fsdp')
- grad_w_down: float32 [3072, 768], P('fsdp')
- grad_b_down: float32 [768], P('fsdp')
The draws below stay inside these ranges and needn't reach their ends.
Inputs may be any that keep to these rules, and one draw needn't show every extreme that they name: `lengths`: each sequence has at least 256 valid tokens, and some sequence fills all 1024 slots.
All inputs are finite; a program needn't handle non-finite values. No bound on the sum of `cells` on one device may be relied on, other than what follows from the above.
Results may differ from the reference program's by a relative error of at most 0.019.
Values may be sent and summed in bfloat16 or wider, within the bound.
A program may use at most 128 MiB of HBM per device.

```python
import math
import jax
import jax.numpy as jnp
from jax import lax

D = 768
H = 12
HD = 64
FF = 3072
CTX = 1024
LEAST = 256
SEQS = 32


def draw_lengths(key, part):
    first_key, second_key = jax.random.split(key)
    uniform_ints = jax.random.randint(first_key, (SEQS,), 0, CTX)
    squared = uniform_ints * uniform_ints // CTX
    spans = LEAST + (CTX - LEAST) * squared // CTX
    longest = jax.random.randint(second_key, (), 0, SEQS)
    return jnp.where(jnp.arange(SEQS) == longest, CTX, spans).astype(jnp.int32)


def set_ends(values, rng, least, high):
    index_at = [jax.random.randint(jax.random.fold_in(rng, axis), (), 0, length) for axis, length in enumerate(values.shape)]
    widest = values.shape.index(max(values.shape))
    neighbour = index_at[:widest] + [(index_at[widest] + 1) % values.shape[widest]] + index_at[widest + 1:]
    return values.at[tuple(index_at)].set(least).at[tuple(neighbour)].set(high)


def spiked(array, key, source, target, shards_of, factor):
    owner, partner = [(jnp.arange(array.shape[dim]) // (array.shape[dim] // shards_of)).reshape([-1 if axis == dim else 1 for axis in range(array.ndim)]) for dim in (source, target)]
    chosen = jax.random.permutation(key, shards_of)[partner]
    strong = (owner == chosen) | (owner == (partner + shards_of // 2) % shards_of)
    return jnp.where(strong, factor * array, array)


def block_levels(key, shape, shards, smallest, high):
    loudness, own = 1.0, jax.random.fold_in(key, 6)
    for position, parts in shards:
        heights = jnp.exp(jax.random.uniform(jax.random.fold_in(own, position), (parts,), jnp.float32, smallest / len(shards), high / len(shards)))
        loudness = loudness * jnp.repeat(heights, shape[position] // parts).reshape([-1 if axis == position else 1 for axis in range(len(shape))])
    return loudness


def normal_values(rng, shape, width, reach, pieces=(), held_as=jnp.bfloat16):
    entries = width * jax.random.normal(rng, shape, jnp.float32)
    if pieces:
        entries = entries * block_levels(rng, shape, pieces, -0.22, 0.18)
    return jnp.clip(entries, -reach, reach).astype(held_as)


def heavy_noise(key, extent, spread, bound, cuts, heavy, kind=jnp.bfloat16):
    array = spread * jax.random.normal(key, extent, jnp.float32)
    if cuts:
        array = array * block_levels(key, extent, cuts, -0.22, 0.18)
    return jnp.clip(spiked(array, jax.random.fold_in(key, 3), *heavy), -bound, bound).astype(kind)


def setup_inputs(seed: int = 0) -> dict:
    keys = jax.random.split(jax.random.key(seed), 18)
    return {
        "tokens": normal_values(keys[0], (SEQS, CTX, D), 1.0, 6.0, ((0, 32),)),
        "lengths": draw_lengths(jax.random.fold_in(keys[17], 71), 0),
        "cells": set_ends((jax.random.randint(keys[2], (SEQS, CTX), 0, 8) < 7).astype(jnp.int32), jax.random.fold_in(keys[2], 1), 0, 1),
        "cotangent": heavy_noise(keys[3], (SEQS, CTX, D), 1.0, 6.0, ((0, 32),), (0, 2, 32, 2.75)),
        "ln1_gain": jnp.clip(1.0 + 0.1 * jax.random.normal(keys[4], (D,), jnp.float32), 0.5, 1.5).astype(jnp.bfloat16),
        "ln1_bias": normal_values(keys[5], (D,), 0.5, 3.0, ((0, 8),)),
        "w_qkv": normal_values(keys[6], (D, 3 * D), D ** -0.5, 0.21875, ((0, 8),)),
        "b_query": normal_values(keys[7], (D,), 1.0, 6.0, ((0, 8),)),
        "b_value": normal_values(keys[8], (D,), 1.0, 6.0, ((0, 8),)),
        "w_out": normal_values(keys[9], (D, D), (D // 16) ** -0.5, 0.875, ((0, 8),)),
        "b_out": normal_values(keys[10], (D,), 0.5, 3.0, ((0, 8),)),
        "ln2_gain": jnp.clip(1.0 + 0.1 * jax.random.normal(keys[11], (D,), jnp.float32), 0.5, 1.5).astype(jnp.bfloat16),
        "ln2_bias": normal_values(keys[12], (D,), 0.5, 3.0, ((0, 8),)),
        "w_up": normal_values(keys[13], (D, FF), D ** -0.5, 0.21875, ((0, 8),)),
        "b_up": normal_values(keys[14], (FF,), 0.5, 3.0, ((0, 8),)),
        "w_down": normal_values(keys[15], (FF, D), FF ** -0.5, 0.109375, ((0, 8),)),
        "b_down": normal_values(keys[16], (D,), 0.5, 3.0, ((0, 8),)),
    }


HIGHEST = lax.Precision.HIGHEST
EPSILON = 1e-05
GELU_C = 0.7978845608028654
GELU_A = 0.044715

@jax.custom_vjp
def low(v):
    return lax.optimization_barrier(v.astype(jnp.bfloat16)).astype(jnp.float32)

@jax.custom_vjp
def low_back(v):
    return v

def low_keep(v):
    return (low(v), None)

def low_pass(kept, grad):
    return (grad,)

def back_keep(v):
    return (v, None)

def back_low(kept, grad):
    return (low(grad),)
low.defvjp(low_keep, low_pass)
low_back.defvjp(back_keep, back_low)

def layer_norm(values, gain, shift):
    row_mean = lax.optimization_barrier(jnp.mean(values, axis=-1, keepdims=True))
    centered = values - row_mean
    variance = lax.optimization_barrier(jnp.mean(centered * centered, axis=-1, keepdims=True))
    return centered * lax.rsqrt(variance + EPSILON) * gain + shift

def gelu_tanh(values):
    return 0.5 * values * (1.0 + jnp.tanh(GELU_C * (values + GELU_A * values * values * values)))

def matmul(left, right):
    return jnp.dot(left, right, precision=HIGHEST)

def allowed_mask(length, cell_row):
    positions = jnp.arange(CTX)
    query_pos = positions[:, None]
    key_pos = positions[None, :]
    usable = (key_pos <= query_pos) & (key_pos < length) & (cell_row[None, :] == 1)
    return usable | (key_pos == query_pos)

def forward(inputs, params, length, cell_row):
    gain_one, shift_one, qkv_weight, bias_query, bias_value, out_weight, bias_out, gain_two, shift_two, up_weight, bias_up, down_weight, bias_down = params
    scale = 1.0 / math.sqrt(HD)
    normed_one = low(layer_norm(inputs, gain_one, shift_one))
    projected = matmul(normed_one, qkv_weight)
    queries = low(low_back((projected[:, :D] + bias_query) * scale)).reshape(CTX, H, HD)
    key_rows = low(low_back(projected[:, D:2 * D])).reshape(CTX, H, HD)
    value_rows = low(low_back(projected[:, 2 * D:] + bias_value)).reshape(CTX, H, HD)
    scores = low_back(jnp.einsum('qhd,khd->hqk', queries, key_rows, precision=HIGHEST))
    scores = jnp.where(allowed_mask(length, cell_row)[None], scores, -1e+30)
    softmax_rows = low(jax.nn.softmax(scores, axis=-1))
    attended = jnp.einsum('hqk,khd->qhd', softmax_rows, value_rows, precision=HIGHEST).reshape(CTX, D)
    attended = low(low_back(attended))
    branch = low_back(matmul(attended, out_weight) + bias_out)
    middle = inputs + branch
    normed_two = low(layer_norm(middle, gain_two, shift_two))
    hidden = low_back(matmul(normed_two, up_weight) + bias_up)
    activated = low(gelu_tanh(hidden))
    mlp_out = low_back(matmul(activated, down_weight) + bias_down)
    return middle + mlp_out

def reference(tokens, lengths, cells, cotangent, ln1_gain, ln1_bias, w_qkv, b_query, b_value, w_out, b_out, ln2_gain, ln2_bias, w_up, b_up, w_down, b_down):
    params = tuple((item.astype(jnp.float32) for item in (ln1_gain, ln1_bias, w_qkv, b_query, b_value, w_out, b_out, ln2_gain, ln2_bias, w_up, b_up, w_down, b_down)))

    def one_sequence(carry, item):
        seq_in, seq_cot, length, cell_row = item
        valid = (jnp.arange(CTX) < length).astype(jnp.float32)

        def layer(inputs, weights):
            return forward(inputs, weights, length, cell_row)
        result, pullback = jax.vjp(layer, seq_in.astype(jnp.float32), params)
        grad_in, grad_params = pullback(seq_cot.astype(jnp.float32) * valid[:, None])
        carry = tuple((total + part for total, part in zip(carry, grad_params)))
        return (carry, (result.astype(jnp.bfloat16), grad_in))
    zeros = tuple((jnp.zeros_like(item) for item in params))
    sums, (results, grad_inputs) = lax.scan(one_sequence, zeros, (tokens, cotangent, lengths, cells))
    return (results, grad_inputs, sums[0], sums[1], sums[2], sums[3], sums[4], sums[5], sums[6], sums[7], sums[8], sums[9], sums[10], sums[11], sums[12])
```

```python
from functools import partial
import math

import jax
import jax.numpy as jnp
from jax import lax
from jax.experimental import pallas as pl
from jax.experimental.pallas import tpu as pltpu
from jax.sharding import PartitionSpec as P

HEADS = 12
EPSILON = 1e-05
GELU_C = 0.7978845608028654
GELU_A = 0.044715
MASKED = -1e30
TILE = 256
VMEM_BYTES = 60 * 1024 * 1024
F32 = jnp.float32
BF16 = jnp.bfloat16


def mm(a, b):
    return jnp.dot(a, b, preferred_element_type=F32)


def mm_nt(a, b):
    return lax.dot_general(a, b, (((1,), (1,)), ((), ())), preferred_element_type=F32)


def mm_tn(a, b):
    return lax.dot_general(a, b, (((0,), (0,)), ((), ())), preferred_element_type=F32)


def params(**kw):
    return pltpu.CompilerParams(
        dimension_semantics=("arbitrary",), vmem_limit_bytes=VMEM_BYTES, **kw
    )


def cost(flops, bytes_accessed, transcendentals=0):
    return pl.CostEstimate(
        flops=int(flops), bytes_accessed=int(bytes_accessed), transcendentals=int(transcendentals)
    )


def norm_forward(values):
    row_mean = jnp.mean(values, axis=-1, keepdims=True)
    centered = values - row_mean
    inv_std = lax.rsqrt(jnp.mean(centered * centered, axis=-1, keepdims=True) + EPSILON)
    return centered * inv_std, inv_std


def norm_backward(grad_normed, normalized, inv_std, gain):
    scaled = grad_normed * gain
    return inv_std * (
        scaled
        - jnp.mean(scaled, axis=-1, keepdims=True)
        - normalized * jnp.mean(scaled * normalized, axis=-1, keepdims=True)
    )


def gelu_pair(u):
    square = u * u
    tanh_part = jnp.tanh(u * (GELU_C + (GELU_C * GELU_A) * square))
    half = 0.5 + 0.5 * tanh_part
    value = u * half
    slope = half + value * (1.0 - tanh_part) * (GELU_C + (3.0 * GELU_C * GELU_A) * square)
    return value, slope


def whole(shape):
    return pl.BlockSpec(shape, lambda i: (0,) * len(shape), pipeline_mode=pl.Buffered(1))


def rows_spec(tile, width):
    return pl.BlockSpec((tile, width), lambda i: (i, 0))


def qkv_kernel(scale, x_ref, w_ref, gain_ref, shift_ref, bq_ref, bv_ref, a1_ref, qkv_ref):
    width = x_ref.shape[1]
    xhat, _ = norm_forward(x_ref[...].astype(F32))
    a1 = (xhat * gain_ref[...] + shift_ref[...]).astype(BF16)
    a1_ref[...] = a1
    q = mm(a1, w_ref[:, 0:width])
    qkv_ref[:, 0:width] = ((q + bq_ref[...]) * scale).astype(BF16)
    k = mm(a1, w_ref[:, width : 2 * width])
    qkv_ref[:, width : 2 * width] = k.astype(BF16)
    v = mm(a1, w_ref[:, 2 * width : 3 * width])
    qkv_ref[:, 2 * width : 3 * width] = (v + bv_ref[...]).astype(BF16)


def qkv_forward(x, w_qkv, gain, shift, bq, bv, scale):
    rows, width = x.shape
    vec = whole((1, width))
    return pl.pallas_call(
        partial(qkv_kernel, scale),
        grid=(rows // TILE,),
        in_specs=[rows_spec(TILE, width), whole(w_qkv.shape), vec, vec, vec, vec],
        out_specs=[rows_spec(TILE, width), rows_spec(TILE, 3 * width)],
        out_shape=[
            jax.ShapeDtypeStruct((rows, width), BF16),
            jax.ShapeDtypeStruct((rows, 3 * width), BF16),
        ],
        compiler_params=params(),
        cost_estimate=cost(6 * rows * width * width, 12 * rows * width),
        name="qkv_forward",
    )(x, w_qkv, gain, shift, bq, bv)


def split3(value):
    first = value.astype(BF16)
    rest = value - first.astype(F32)
    second = rest.astype(BF16)
    third = (rest - second.astype(F32)).astype(BF16)
    return first, second, third


def attn_fwd_kernel(q_ref, k_ref, v_ref, kbias_ref, rbias_ref, o_ref, qa_ref, mask_ref):
    blocks = q_ref.shape[0] // TILE
    lane = lax.broadcasted_iota(jnp.int32, (1, 128), 1)

    @pl.when(pl.program_id(0) == 0)
    def _():
        row = lax.broadcasted_iota(jnp.int32, (TILE, TILE), 0)
        col = lax.broadcasted_iota(jnp.int32, (TILE, TILE), 1)
        for i in range(blocks):
            usable = rbias_ref[:, i * TILE : (i + 1) * TILE]
            mask_ref[i] = jnp.where(row == col, 0.0, jnp.where(row > col, usable, MASKED))

    zero = jnp.zeros((), BF16)
    one = jnp.ones((), BF16)
    for head in range(2):
        base = 64 * head
        extra = 64 - base
        own = (lane >= base) & (lane < base + 64)
        k_off = jnp.where(own, k_ref[...], jnp.where(lane == extra, kbias_ref[...], zero))
        for i in range(blocks):
            here = slice(i * TILE, (i + 1) * TILE)
            q = jnp.where(own, q_ref[here, :], zero)
            q_off = jnp.where(lane == extra, one, q)
            s_diag = mm_nt(q, k_ref[here, :]) + mask_ref[i]
            row_max = jnp.max(s_diag, axis=-1, keepdims=True)
            if i:
                s_off = mm_nt(q_off, k_off[: i * TILE])
                row_max = jnp.maximum(row_max, jnp.max(s_off, axis=-1, keepdims=True))
            e_diag = jnp.exp(s_diag - row_max)
            total = jnp.sum(e_diag, axis=-1, keepdims=True)
            o = mm(e_diag.astype(BF16), v_ref[here, :])
            if i:
                e_off = jnp.exp(s_off - row_max)
                total += jnp.sum(e_off, axis=-1, keepdims=True)
                o += mm(e_off.astype(BF16), v_ref[0 : i * TILE, :])
            o = (o * (1.0 / total)).astype(BF16)
            if head:
                o_ref[here, :] = jnp.where(own, o, o_ref[here, :])
            else:
                o_ref[here, :] = o
            first, second, third = split3(-(row_max + jnp.log(total)))
            qa = jnp.where(lane == extra + 1, first, q_off)
            qa = jnp.where(lane == extra + 2, second, qa)
            qa = jnp.where(lane == extra + 3, third, qa)
            qa_ref[here, 128 * head : 128 * head + 128] = qa


def attn_forward(qkv, kbias, rbias):
    rows = qkv.shape[0]
    width = qkv.shape[1] // 3
    pairs = width // 128

    def part(p):
        return pl.BlockSpec((rows, 128), lambda i: (0, p * pairs + i))

    return pl.pallas_call(
        attn_fwd_kernel,
        grid=(pairs,),
        in_specs=[part(0), part(1), part(2), whole(kbias.shape), whole(rbias.shape)],
        out_specs=[part(0), pl.BlockSpec((rows, 256), lambda i: (0, i))],
        out_shape=[
            jax.ShapeDtypeStruct((rows, width), BF16),
            jax.ShapeDtypeStruct((rows, 2 * width), BF16),
        ],
        scratch_shapes=[pltpu.VMEM((rows // TILE, TILE, TILE), F32)],
        compiler_params=params(),
        cost_estimate=cost(8 * rows * rows * width, 12 * rows * width),
        name="attn_forward",
    )(qkv, qkv, qkv, kbias, rbias)


def attn_bwd_kernel(
    qa_ref, k_ref, v_ref, o_ref, do_ref, kbias_ref, dq_ref, dk_ref, dv_ref, mask_ref, doa_ref, dqt_ref
):
    rows = k_ref.shape[0]
    blocks = rows // TILE
    lane = lax.broadcasted_iota(jnp.int32, (1, 128), 1)

    @pl.when(pl.program_id(0) == 0)
    def _():
        key = lax.broadcasted_iota(jnp.int32, (TILE, TILE), 0)
        query = lax.broadcasted_iota(jnp.int32, (TILE, TILE), 1)
        for i in range(blocks):
            usable = kbias_ref[i * TILE : (i + 1) * TILE, 0:1].astype(F32)
            mask_ref[i] = jnp.where(key == query, 0.0, jnp.where(query > key, usable, MASKED))

    zero = jnp.zeros((), BF16)
    one = jnp.ones((), BF16)
    product = do_ref[...].astype(F32) * o_ref[...].astype(F32)
    kt = k_ref[...].T
    for head in range(2):
        base = 64 * head
        extra = 64 - base
        own = (lane >= base) & (lane < base + 64)
        terms = (lane > extra) & (lane <= extra + 3)
        qa_cols = slice(128 * head, 128 * head + 128)
        inner = -jnp.sum(jnp.where(own, product, 0.0), axis=-1, keepdims=True)
        first, second, third = split3(inner)
        doa = jnp.where(own, do_ref[...], zero)
        doa = jnp.where(lane == extra + 1, first, doa)
        doa = jnp.where(lane == extra + 2, second, doa)
        doa_ref[...] = jnp.where(lane == extra + 3, third, doa)
        for j in range(blocks):
            here = slice(j * TILE, (j + 1) * TILE)
            after = slice((j + 1) * TILE, rows)
            k_diag = jnp.where(own, k_ref[here, :], jnp.where(terms, one, zero))
            v_aug = jnp.where(own, v_ref[here, :], jnp.where(terms, one, zero))
            p_diag = jnp.exp(mm_nt(k_diag, qa_ref[here, qa_cols]) + mask_ref[j])
            dp_diag = mm_nt(v_aug, doa_ref[here, :])
            ds_diag = (p_diag * dp_diag).astype(BF16)
            dv = mm(p_diag.astype(BF16), do_ref[here, :])
            dk = mm(ds_diag, qa_ref[here, qa_cols])
            dq_diag = mm(kt[:, here], ds_diag)
            if j:
                dqt_ref[:, here] += dq_diag
            else:
                dqt_ref[:, here] = dq_diag
            if j + 1 < blocks:
                k_off = jnp.where(lane == extra, kbias_ref[here, :], k_diag)
                p_off = jnp.exp(mm_nt(k_off, qa_ref[after, qa_cols]))
                dp_off = mm_nt(v_aug, doa_ref[after, :])
                ds_off = (p_off * dp_off).astype(BF16)
                dv += mm(p_off.astype(BF16), do_ref[after, :])
                dk += mm(ds_off, qa_ref[after, qa_cols])
                dq_off = mm(kt[:, here], ds_off)
                if j:
                    dqt_ref[:, after] += dq_off
                else:
                    dqt_ref[:, after] = dq_off
            dk = dk.astype(BF16)
            dv = dv.astype(BF16)
            if head:
                dk_ref[here, :] = jnp.where(own, dk, dk_ref[here, :])
                dv_ref[here, :] = jnp.where(own, dv, dv_ref[here, :])
            else:
                dk_ref[here, :] = dk
                dv_ref[here, :] = dv
        dq = (dqt_ref[...] * 0.125).astype(BF16).T
        if head:
            dq_ref[...] = jnp.where(own, dq, dq_ref[...])
        else:
            dq_ref[...] = dq


def attn_backward(qa, qkv, o, do, kbias, first_pair, pair_count):
    rows, width = o.shape
    pairs = width // 128

    def part(p):
        return pl.BlockSpec((rows, 128), lambda i: (0, p * pairs + first_pair + i))

    out = pl.BlockSpec((rows, 128), lambda i: (0, i))
    shape = jax.ShapeDtypeStruct((rows, 128 * pair_count), BF16)
    return pl.pallas_call(
        attn_bwd_kernel,
        grid=(pair_count,),
        in_specs=[
            pl.BlockSpec((rows, 256), lambda i: (0, first_pair + i)),
            part(1),
            part(2),
            part(0),
            part(0),
            whole(kbias.shape),
        ],
        out_specs=[out, out, out],
        out_shape=[shape, shape, shape],
        scratch_shapes=[
            pltpu.VMEM((rows // TILE, TILE, TILE), F32),
            pltpu.VMEM((rows, 128), BF16),
            pltpu.VMEM((128, rows), F32),
        ],
        compiler_params=params(),
        cost_estimate=cost(20 * rows * rows * 128 * pair_count, 18 * rows * 128 * pair_count),
        name="attn_backward",
    )(qa, qkv, qkv, o, do, kbias)


def mlp_kernel(
    x_ref, o_ref, cot_ref, valid_ref, wo_ref, wu_ref, wd_ref, bo_ref, gain_ref, shift_ref, bu_ref, bd_ref,
    out_ref, dm_ref, a2_ref, g_ref, du_ref, dr_ref, dy_ref, do_ref,
    s_gain_ref, s_shift_ref, s_bu_ref, s_bd_ref, s_bo_ref,
):
    chunk = 768
    hidden = wu_ref.shape[1]
    middle = x_ref[...].astype(F32) + mm(o_ref[...], wo_ref[...]) + bo_ref[...]
    xhat, inv_std = norm_forward(middle)
    a2 = (xhat * gain_ref[...] + shift_ref[...]).astype(BF16)
    a2_ref[...] = a2
    dout = cot_ref[...].astype(F32) * valid_ref[:, 0:1]
    dm = dout.astype(BF16)
    dm_ref[...] = dm
    out = middle + bd_ref[...]
    da2 = jnp.zeros_like(middle)
    first = pl.program_id(0) == 0

    def add_sum(ref, cols, value):
        part = jnp.sum(value, axis=0, keepdims=True)
        ref[:, cols] = jnp.where(first, part, ref[:, cols] + part)

    for c in range(hidden // chunk):
        cols = slice(c * chunk, (c + 1) * chunk)
        u = mm(a2, wu_ref[:, cols]) + bu_ref[:, cols]
        value, slope = gelu_pair(u)
        g = value.astype(BF16)
        g_ref[:, cols] = g
        out += mm(g, wd_ref[cols, :])
        du = (mm_nt(dm, wd_ref[cols, :]) * slope).astype(BF16)
        du_ref[:, cols] = du
        add_sum(s_bu_ref, cols, du.astype(F32))
        da2 += mm_nt(du, wu_ref[:, cols])
    out_ref[...] = out.astype(BF16)
    every = slice(None)
    add_sum(s_bd_ref, every, dm.astype(F32))
    add_sum(s_gain_ref, every, da2 * xhat)
    add_sum(s_shift_ref, every, da2)
    dr = dout + norm_backward(da2, xhat, inv_std, gain_ref[...])
    dr_ref[...] = dr
    dy = dr.astype(BF16)
    dy_ref[...] = dy
    add_sum(s_bo_ref, every, dy.astype(F32))
    do_ref[...] = mm_nt(dy, wo_ref[...]).astype(BF16)


def mlp_both(x, o, cot, valid, w_out, w_up, w_down, b_out, gain, shift, b_up, b_down):
    rows, width = x.shape
    hidden = w_up.shape[1]
    row = rows_spec(TILE, width)
    wide = rows_spec(TILE, hidden)
    vec = whole((1, width))
    vec_wide = whole((1, hidden))
    acc = pl.BlockSpec((1, width), lambda i: (0, 0))
    acc_wide = pl.BlockSpec((1, hidden), lambda i: (0, 0))

    def shape(r, c, t):
        return jax.ShapeDtypeStruct((r, c), t)

    return pl.pallas_call(
        mlp_kernel,
        grid=(rows // TILE,),
        in_specs=[
            row, row, row, rows_spec(TILE, 128),
            whole(w_out.shape), whole(w_up.shape), whole(w_down.shape),
            vec, vec, vec, vec_wide, vec,
        ],
        out_specs=[row, row, row, wide, wide, row, row, row, acc, acc, acc_wide, acc, acc],
        out_shape=[
            shape(rows, width, BF16), shape(rows, width, BF16), shape(rows, width, BF16),
            shape(rows, hidden, BF16), shape(rows, hidden, BF16), shape(rows, width, F32),
            shape(rows, width, BF16), shape(rows, width, BF16),
            shape(1, width, F32), shape(1, width, F32), shape(1, hidden, F32),
            shape(1, width, F32), shape(1, width, F32),
        ],
        compiler_params=params(),
        cost_estimate=cost(rows * width * (8 * hidden + 4 * width), 24 * rows * width + 12 * rows * hidden),
        name="mlp_both",
    )(x, o, cot, valid, w_out, w_up, w_down, b_out, gain, shift, b_up, b_down)


def grad_kernel(tall, a_ref, *refs):
    out_ref = refs[-1]
    out_ref[...] = mm_tn(a_ref[...], refs[0][...]).astype(BF16)


def weight_grad(a, b, name):
    rows, m = a.shape
    n = b.shape[1]
    tall = m > n
    tile = 512 if max(m, n) % 512 == 0 else 384
    tile = min(tile, max(m, n))
    if tall:
        specs = [pl.BlockSpec((rows, tile), lambda i: (0, i)), whole(b.shape)]
        out = pl.BlockSpec((tile, n), lambda i: (i, 0))
    else:
        specs = [whole(a.shape), pl.BlockSpec((rows, tile), lambda i: (0, i))]
        out = pl.BlockSpec((m, tile), lambda i: (0, i))
    return pl.pallas_call(
        partial(grad_kernel, tall),
        grid=(max(m, n) // tile,),
        in_specs=specs,
        out_specs=out,
        out_shape=jax.ShapeDtypeStruct((m, n), BF16),
        compiler_params=params(),
        cost_estimate=cost(2 * rows * m * n, 2 * (rows * (m + n) + m * n)),
        name=name,
    )(a, b)


def input_kernel(
    x_ref, dq_ref, dk_ref, dv_ref, dr_ref, w_ref, gain_ref, out_ref, s_gain_ref, s_shift_ref, s_bq_ref, s_bv_ref
):
    width = x_ref.shape[1]
    xhat, inv_std = norm_forward(x_ref[...].astype(F32))
    da = mm_nt(dq_ref[...], w_ref[:, 0:width])
    da += mm_nt(dk_ref[...], w_ref[:, width : 2 * width])
    da += mm_nt(dv_ref[...], w_ref[:, 2 * width : 3 * width])
    first = pl.program_id(0) == 0

    def add_sum(ref, value):
        part = jnp.sum(value, axis=0, keepdims=True)
        ref[...] = jnp.where(first, part, ref[...] + part)

    add_sum(s_gain_ref, da * xhat)
    add_sum(s_shift_ref, da)
    add_sum(s_bq_ref, dq_ref[...].astype(F32))
    add_sum(s_bv_ref, dv_ref[...].astype(F32))
    out_ref[...] = dr_ref[...] + norm_backward(da, xhat, inv_std, gain_ref[...])


def input_grad(x, dq, dk, dv, dr, w_qkv, gain):
    rows, width = x.shape
    row = rows_spec(TILE, width)
    acc = pl.BlockSpec((1, width), lambda i: (0, 0))
    vec = jax.ShapeDtypeStruct((1, width), F32)
    return pl.pallas_call(
        input_kernel,
        grid=(rows // TILE,),
        in_specs=[row, row, row, row, row, whole(w_qkv.shape), whole((1, width))],
        out_specs=[row, acc, acc, acc, acc],
        out_shape=[jax.ShapeDtypeStruct((rows, width), F32), vec, vec, vec, vec],
        compiler_params=params(),
        cost_estimate=cost(6 * rows * width * width, 16 * rows * width),
        name="input_grad",
    )(x, dq, dk, dv, dr, w_qkv, gain)


def mask_terms(lengths, cells, context):
    usable = (jnp.arange(context) < lengths[0]) & (cells[0] == 1)
    bias = jnp.where(usable, 0.0, MASKED)
    kbias = jnp.broadcast_to(bias.astype(BF16)[:, None], (context, 128))
    rbias = bias[None, :]
    valid = jnp.broadcast_to(
        (jnp.arange(context) < lengths[0]).astype(F32)[:, None], (context, 128)
    )
    return kbias, rbias, valid


def gather(x):
    return lax.all_gather(x, "fsdp", axis=0, tiled=True)


def reduce_rows(x):
    rows = lax.psum_scatter(x, "fsdp", scatter_dimension=0, tiled=True)
    return lax.psum(rows, "dp").astype(F32)


def per_device(
    tokens, lengths, cells, cotangent, ln1_gain, ln1_bias, w_qkv, b_query, b_value, w_out, b_out,
    ln2_gain, ln2_bias, w_up, b_up, w_down, b_down,
):
    seqs, context, width = tokens.shape
    vectors = (ln1_gain, ln1_bias, b_query, b_value, b_out, ln2_gain, ln2_bias, b_down, b_up)
    sizes = [v.shape[0] for v in vectors]
    packed = lax.all_gather(jnp.concatenate(vectors), "fsdp", axis=0).astype(F32)
    edges = [sum(sizes[:i]) for i in range(len(sizes) + 1)]
    g1, h1, bq, bv, bo, g2, h2, bd, bu = (
        packed[:, a:b].reshape(1, -1) for a, b in zip(edges[:-1], edges[1:])
    )
    qkv_full = gather(w_qkv)
    out_full = gather(w_out)
    up_full = gather(w_up)
    down_full = gather(w_down)
    x = tokens[0]
    kbias, rbias, valid = mask_terms(lengths, cells, context)
    a1, qkv = qkv_forward(x, qkv_full, g1, h1, bq, bv, 0.125)
    o, qa = attn_forward(qkv, kbias, rbias)
    out, dm, a2, g, du, dr, dy, do, s_g2, s_h2, s_bu, s_bd, s_bo = mlp_both(
        x, o, cotangent[0], valid, out_full, up_full, down_full, bo, g2, h2, bu, bd
    )
    grad_down = reduce_rows(weight_grad(g, dm, "grad_down"))
    grad_up = reduce_rows(weight_grad(a2, du, "grad_up"))
    grad_out = reduce_rows(weight_grad(o, dy, "grad_out"))
    dq, dk, dv = attn_backward(qa, qkv, o, do, kbias, 0, width // 128)
    grad_qkv = reduce_rows(
        jnp.concatenate([weight_grad(a1, t, "grad_qkv") for t in (dq, dk, dv)], axis=1)
    )
    grad_x, s_g1, s_h1, s_bq, s_bv = input_grad(x, dq, dk, dv, dr, qkv_full, g1)
    shards = packed.shape[0]
    sums = jnp.concatenate(
        [s.reshape(shards, -1) for s in (s_g1, s_h1, s_bq, s_bv, s_bo, s_g2, s_h2, s_bd, s_bu)], axis=1
    )
    mine = lax.psum(sums, ("dp", "fsdp"))[lax.axis_index("fsdp")]
    g_g1, g_h1, g_bq, g_bv, g_bo, g_g2, g_h2, g_bd, g_bu = (
        mine[a:b] for a, b in zip(edges[:-1], edges[1:])
    )
    return (
        out[None], grad_x[None], g_g1, g_h1, grad_qkv, g_bq, g_bv, grad_out, g_bo, g_g2, g_h2,
        grad_up, g_bu, grad_down, g_bd,
    )


def solution(mesh):
    split = P(("dp", "fsdp"), None, None)
    vec, mat = P("fsdp"), P("fsdp", None)
    in_specs = (
        split, P(("dp", "fsdp")), P(("dp", "fsdp"), None), split,
        vec, vec, mat, vec, vec, mat, vec, vec, vec, mat, vec, mat, vec,
    )
    out_specs = (split, split, vec, vec, mat, vec, vec, mat, vec, vec, vec, mat, vec, mat, vec)
    return jax.shard_map(
        per_device, mesh=mesh, in_specs=in_specs, out_specs=out_specs, check_vma=False
    )
```

```python
from functools import partial
import math

import jax
import jax.numpy as jnp
from jax import lax
from jax.experimental import pallas as pl
from jax.experimental.pallas import tpu as pltpu
from jax.sharding import PartitionSpec as P

HEADS = 12
EPSILON = 1e-05
GELU_C = 0.7978845608028654
GELU_A = 0.044715
MASKED = -1e30
TILE = 256
VMEM_BYTES = 60 * 1024 * 1024
F32 = jnp.float32
BF16 = jnp.bfloat16


def mm(a, b):
    return jnp.dot(a, b, preferred_element_type=F32)


def mm_nt(a, b):
    return lax.dot_general(a, b, (((1,), (1,)), ((), ())), preferred_element_type=F32)


def mm_tn(a, b):
    return lax.dot_general(a, b, (((0,), (0,)), ((), ())), preferred_element_type=F32)


def params(**kw):
    return pltpu.CompilerParams(
        dimension_semantics=("arbitrary",), vmem_limit_bytes=VMEM_BYTES, **kw
    )


def cost(flops, bytes_accessed, transcendentals=0):
    return pl.CostEstimate(
        flops=int(flops), bytes_accessed=int(bytes_accessed), transcendentals=int(transcendentals)
    )


def norm_forward(values):
    row_mean = jnp.mean(values, axis=-1, keepdims=True)
    centered = values - row_mean
    inv_std = lax.rsqrt(jnp.mean(centered * centered, axis=-1, keepdims=True) + EPSILON)
    return centered * inv_std, inv_std


def norm_backward(grad_normed, normalized, inv_std, gain):
    scaled = grad_normed * gain
    return inv_std * (
        scaled
        - jnp.mean(scaled, axis=-1, keepdims=True)
        - normalized * jnp.mean(scaled * normalized, axis=-1, keepdims=True)
    )


def gelu_pair(u):
    square = u * u
    tanh_part = jnp.tanh(u * (GELU_C + (GELU_C * GELU_A) * square))
    half = 0.5 + 0.5 * tanh_part
    value = u * half
    slope = half + value * (1.0 - tanh_part) * (GELU_C + (3.0 * GELU_C * GELU_A) * square)
    return value, slope


def whole(shape):
    return pl.BlockSpec(shape, lambda i: (0,) * len(shape), pipeline_mode=pl.Buffered(1))


def rows_spec(tile, width):
    return pl.BlockSpec((tile, width), lambda i: (i, 0))


def qkv_kernel(scale, x_ref, w_ref, vec_ref, a1_ref, qkv_ref):
    width = x_ref.shape[1]
    gain, shift, bq, bv = (vec_ref[i : i + 1, :] for i in range(4))
    xhat, _ = norm_forward(x_ref[...].astype(F32))
    a1 = (xhat * gain + shift).astype(BF16)
    a1_ref[...] = a1
    q = mm(a1, w_ref[0])
    qkv_ref[:, 0:width] = ((q + bq) * scale).astype(BF16)
    k = mm(a1, w_ref[1])
    qkv_ref[:, width : 2 * width] = k.astype(BF16)
    v = mm(a1, w_ref[2])
    qkv_ref[:, 2 * width : 3 * width] = (v + bv).astype(BF16)


def qkv_forward(x, ab, vecs, scale):
    rows, width = x.shape
    return pl.pallas_call(
        partial(qkv_kernel, scale),
        grid=(rows // TILE,),
        in_specs=[rows_spec(TILE, width), whole((3, width, width)), whole(vecs.shape)],
        out_specs=[rows_spec(TILE, width), rows_spec(TILE, 3 * width)],
        out_shape=[
            jax.ShapeDtypeStruct((rows, width), BF16),
            jax.ShapeDtypeStruct((rows, 3 * width), BF16),
        ],
        compiler_params=params(),
        cost_estimate=cost(6 * rows * width * width, 12 * rows * width),
        name="qkv_forward",
    )(x, ab, vecs)


def split3(value):
    first = value.astype(BF16)
    rest = value - first.astype(F32)
    second = rest.astype(BF16)
    third = (rest - second.astype(F32)).astype(BF16)
    return first, second, third


def attn_fwd_kernel(q_ref, k_ref, v_ref, kbias_ref, rbias_ref, o_ref, qa_ref, mask_ref):
    blocks = q_ref.shape[0] // TILE
    lane = lax.broadcasted_iota(jnp.int32, (1, 128), 1)

    @pl.when(pl.program_id(0) == 0)
    def _():
        row = lax.broadcasted_iota(jnp.int32, (TILE, TILE), 0)
        col = lax.broadcasted_iota(jnp.int32, (TILE, TILE), 1)
        for i in range(blocks):
            usable = rbias_ref[:, i * TILE : (i + 1) * TILE]
            mask_ref[i] = jnp.where(row == col, 0.0, jnp.where(row > col, usable, MASKED))

    zero = jnp.zeros((), BF16)
    one = jnp.ones((), BF16)
    for head in range(2):
        base = 64 * head
        extra = 64 - base
        own = (lane >= base) & (lane < base + 64)
        k_off = jnp.where(own, k_ref[...], jnp.where(lane == extra, kbias_ref[...], zero))
        for i in range(blocks):
            here = slice(i * TILE, (i + 1) * TILE)
            q = jnp.where(own, q_ref[here, :], zero)
            q_off = jnp.where(lane == extra, one, q)
            s_diag = mm_nt(q, k_ref[here, :]) + mask_ref[i]
            row_max = jnp.max(s_diag, axis=-1, keepdims=True)
            if i:
                s_off = mm_nt(q_off, k_off[: i * TILE])
                row_max = jnp.maximum(row_max, jnp.max(s_off, axis=-1, keepdims=True))
            e_diag = jnp.exp(s_diag - row_max)
            total = jnp.sum(e_diag, axis=-1, keepdims=True)
            o = mm(e_diag.astype(BF16), v_ref[here, :])
            if i:
                e_off = jnp.exp(s_off - row_max)
                total += jnp.sum(e_off, axis=-1, keepdims=True)
                o += mm(e_off.astype(BF16), v_ref[0 : i * TILE, :])
            o = (o * (1.0 / total)).astype(BF16)
            if head:
                o_ref[here, :] = jnp.where(own, o, o_ref[here, :])
            else:
                o_ref[here, :] = o
            first, second, third = split3(-(row_max + jnp.log(total)))
            qa = jnp.where(lane == extra + 1, first, q_off)
            qa = jnp.where(lane == extra + 2, second, qa)
            qa = jnp.where(lane == extra + 3, third, qa)
            qa_ref[here, 128 * head : 128 * head + 128] = qa


def attn_forward(qkv, kbias, rbias):
    rows = qkv.shape[0]
    width = qkv.shape[1] // 3
    pairs = width // 128

    def part(p):
        return pl.BlockSpec((rows, 128), lambda i: (0, p * pairs + i))

    return pl.pallas_call(
        attn_fwd_kernel,
        grid=(pairs,),
        in_specs=[part(0), part(1), part(2), whole(kbias.shape), whole(rbias.shape)],
        out_specs=[part(0), pl.BlockSpec((rows, 256), lambda i: (0, i))],
        out_shape=[
            jax.ShapeDtypeStruct((rows, width), BF16),
            jax.ShapeDtypeStruct((rows, 2 * width), BF16),
        ],
        scratch_shapes=[pltpu.VMEM((rows // TILE, TILE, TILE), F32)],
        compiler_params=params(),
        cost_estimate=cost(8 * rows * rows * width, 12 * rows * width),
        name="attn_forward",
    )(qkv, qkv, qkv, kbias, rbias)


def attn_bwd_kernel(
    qa_ref, k_ref, v_ref, o_ref, do_ref, kbias_ref, dq_ref, dk_ref, dv_ref, mask_ref, doa_ref, dqt_ref
):
    rows = k_ref.shape[0]
    blocks = rows // TILE
    lane = lax.broadcasted_iota(jnp.int32, (1, 128), 1)

    @pl.when(pl.program_id(0) == 0)
    def _():
        key = lax.broadcasted_iota(jnp.int32, (TILE, TILE), 0)
        query = lax.broadcasted_iota(jnp.int32, (TILE, TILE), 1)
        for i in range(blocks):
            usable = kbias_ref[i * TILE : (i + 1) * TILE, 0:1].astype(F32)
            mask_ref[i] = jnp.where(key == query, 0.0, jnp.where(query > key, usable, MASKED))

    zero = jnp.zeros((), BF16)
    one = jnp.ones((), BF16)
    product = do_ref[...].astype(F32) * o_ref[...].astype(F32)
    kt = k_ref[...].T
    for head in range(2):
        base = 64 * head
        extra = 64 - base
        own = (lane >= base) & (lane < base + 64)
        terms = (lane > extra) & (lane <= extra + 3)
        qa_cols = slice(128 * head, 128 * head + 128)
        inner = -jnp.sum(jnp.where(own, product, 0.0), axis=-1, keepdims=True)
        first, second, third = split3(inner)
        doa = jnp.where(own, do_ref[...], zero)
        doa = jnp.where(lane == extra + 1, first, doa)
        doa = jnp.where(lane == extra + 2, second, doa)
        doa_ref[...] = jnp.where(lane == extra + 3, third, doa)
        for j in range(blocks):
            here = slice(j * TILE, (j + 1) * TILE)
            after = slice((j + 1) * TILE, rows)
            k_diag = jnp.where(own, k_ref[here, :], jnp.where(terms, one, zero))
            v_aug = jnp.where(own, v_ref[here, :], jnp.where(terms, one, zero))
            p_diag = jnp.exp(mm_nt(k_diag, qa_ref[here, qa_cols]) + mask_ref[j])
            dp_diag = mm_nt(v_aug, doa_ref[here, :])
            ds_diag = (p_diag * dp_diag).astype(BF16)
            dv = mm(p_diag.astype(BF16), do_ref[here, :])
            dk = mm(ds_diag, qa_ref[here, qa_cols])
            dq_diag = mm(kt[:, here], ds_diag)
            if j:
                dqt_ref[:, here] += dq_diag
            else:
                dqt_ref[:, here] = dq_diag
            if j + 1 < blocks:
                k_off = jnp.where(lane == extra, kbias_ref[here, :], k_diag)
                p_off = jnp.exp(mm_nt(k_off, qa_ref[after, qa_cols]))
                dp_off = mm_nt(v_aug, doa_ref[after, :])
                ds_off = (p_off * dp_off).astype(BF16)
                dv += mm(p_off.astype(BF16), do_ref[after, :])
                dk += mm(ds_off, qa_ref[after, qa_cols])
                dq_off = mm(kt[:, here], ds_off)
                if j:
                    dqt_ref[:, after] += dq_off
                else:
                    dqt_ref[:, after] = dq_off
            dk = dk.astype(BF16)
            dv = dv.astype(BF16)
            if head:
                dk_ref[here, :] = jnp.where(own, dk, dk_ref[here, :])
                dv_ref[here, :] = jnp.where(own, dv, dv_ref[here, :])
            else:
                dk_ref[here, :] = dk
                dv_ref[here, :] = dv
        dq = (dqt_ref[...] * 0.125).astype(BF16).T
        if head:
            dq_ref[...] = jnp.where(own, dq, dq_ref[...])
        else:
            dq_ref[...] = dq


def attn_backward(qa, qkv, o, do, kbias, first_pair, pair_count):
    rows, width = o.shape
    pairs = width // 128

    def part(p):
        return pl.BlockSpec((rows, 128), lambda i: (0, p * pairs + first_pair + i))

    out = pl.BlockSpec((rows, 128), lambda i: (0, i))
    shape = jax.ShapeDtypeStruct((rows, 128 * pair_count), BF16)
    return pl.pallas_call(
        attn_bwd_kernel,
        grid=(pair_count,),
        in_specs=[
            pl.BlockSpec((rows, 256), lambda i: (0, first_pair + i)),
            part(1),
            part(2),
            part(0),
            part(0),
            whole(kbias.shape),
        ],
        out_specs=[out, out, out],
        out_shape=[shape, shape, shape],
        scratch_shapes=[
            pltpu.VMEM((rows // TILE, TILE, TILE), F32),
            pltpu.VMEM((rows, 128), BF16),
            pltpu.VMEM((128, rows), F32),
        ],
        compiler_params=params(),
        cost_estimate=cost(20 * rows * rows * 128 * pair_count, 18 * rows * 128 * pair_count),
        name="attn_backward",
    )(qa, qkv, qkv, o, do, kbias)


def mlp_kernel(
    x_ref, o_ref, cot_ref, valid_ref, wo_ref, wu_ref, wd_ref, vec_ref, bu_ref,
    out_ref, dm_ref, a2_ref, g_ref, du_ref, dr_ref, dy_ref, do_ref,
    s_gain_ref, s_shift_ref, s_bu_ref, s_bd_ref, s_bo_ref,
):
    chunk = wu_ref.shape[2]
    hidden = wd_ref.shape[0]
    bo, gain, shift, bd = (vec_ref[i : i + 1, :] for i in range(4, 8))
    middle = x_ref[...].astype(F32) + mm(o_ref[...], wo_ref[0]) + bo
    xhat, inv_std = norm_forward(middle)
    a2 = (xhat * gain + shift).astype(BF16)
    a2_ref[...] = a2
    dout = cot_ref[...].astype(F32) * valid_ref[:, 0:1]
    dm = dout.astype(BF16)
    dm_ref[...] = dm
    out = middle + bd
    da2 = jnp.zeros_like(middle)
    first = pl.program_id(0) == 0

    def add_sum(ref, cols, value):
        part = jnp.sum(value, axis=0, keepdims=True)
        ref[:, cols] = jnp.where(first, part, ref[:, cols] + part)

    for c in range(hidden // chunk):
        cols = slice(c * chunk, (c + 1) * chunk)
        u = mm(a2, wu_ref[c]) + bu_ref[:, cols]
        value, slope = gelu_pair(u)
        g = value.astype(BF16)
        g_ref[:, cols] = g
        out += mm(g, wd_ref[cols, :])
        du = (mm_nt(dm, wd_ref[cols, :]) * slope).astype(BF16)
        du_ref[:, cols] = du
        add_sum(s_bu_ref, cols, du.astype(F32))
        da2 += mm_nt(du, wu_ref[c])
    out_ref[...] = out.astype(BF16)
    every = slice(None)
    add_sum(s_bd_ref, every, dm.astype(F32))
    add_sum(s_gain_ref, every, da2 * xhat)
    add_sum(s_shift_ref, every, da2)
    dr = dout + norm_backward(da2, xhat, inv_std, gain)
    dr_ref[...] = dr
    dy = dr.astype(BF16)
    dy_ref[...] = dy
    add_sum(s_bo_ref, every, dy.astype(F32))
    do_ref[...] = mm_nt(dy, wo_ref[0]).astype(BF16)


def mlp_both(x, o, cot, valid, ab, w_down, vecs, b_up):
    rows, width = x.shape
    hidden = w_down.shape[0]
    row = rows_spec(TILE, width)
    wide = rows_spec(TILE, hidden)
    acc = pl.BlockSpec((1, width), lambda i: (0, 0))
    acc_wide = pl.BlockSpec((1, hidden), lambda i: (0, 0))

    def shape(r, c, t):
        return jax.ShapeDtypeStruct((r, c), t)

    return pl.pallas_call(
        mlp_kernel,
        grid=(rows // TILE,),
        in_specs=[
            row, row, row, rows_spec(TILE, 128),
            pl.BlockSpec((1, width, width), lambda i: (3, 0, 0), pipeline_mode=pl.Buffered(1)),
            pl.BlockSpec((4, width, width), lambda i: (1, 0, 0), pipeline_mode=pl.Buffered(1)),
            whole(w_down.shape), whole(vecs.shape), whole(b_up.shape),
        ],
        out_specs=[row, row, row, wide, wide, row, row, row, acc, acc, acc_wide, acc, acc],
        out_shape=[
            shape(rows, width, BF16), shape(rows, width, BF16), shape(rows, width, BF16),
            shape(rows, hidden, BF16), shape(rows, hidden, BF16), shape(rows, width, F32),
            shape(rows, width, BF16), shape(rows, width, BF16),
            shape(1, width, F32), shape(1, width, F32), shape(1, hidden, F32),
            shape(1, width, F32), shape(1, width, F32),
        ],
        compiler_params=params(),
        cost_estimate=cost(rows * width * (8 * hidden + 4 * width), 24 * rows * width + 12 * rows * hidden),
        name="mlp_both",
    )(x, o, cot, valid, ab, ab, w_down, vecs, b_up)


def input_kernel(
    x_ref, dq_ref, dk_ref, dv_ref, dr_ref, w_ref, vec_ref, out_ref, s_gain_ref, s_shift_ref, s_bq_ref, s_bv_ref
):
    width = x_ref.shape[1]
    xhat, inv_std = norm_forward(x_ref[...].astype(F32))
    da = mm_nt(dq_ref[...], w_ref[0])
    da += mm_nt(dk_ref[...], w_ref[1])
    da += mm_nt(dv_ref[...], w_ref[2])
    first = pl.program_id(0) == 0

    def add_sum(ref, value):
        part = jnp.sum(value, axis=0, keepdims=True)
        ref[...] = jnp.where(first, part, ref[...] + part)

    add_sum(s_gain_ref, da * xhat)
    add_sum(s_shift_ref, da)
    add_sum(s_bq_ref, dq_ref[...].astype(F32))
    add_sum(s_bv_ref, dv_ref[...].astype(F32))
    out_ref[...] = dr_ref[...] + norm_backward(da, xhat, inv_std, vec_ref[0:1, :])


def input_grad(x, dq, dk, dv, dr, ab, vecs):
    rows, width = x.shape
    row = rows_spec(TILE, width)
    acc = pl.BlockSpec((1, width), lambda i: (0, 0))
    vec = jax.ShapeDtypeStruct((1, width), F32)
    return pl.pallas_call(
        input_kernel,
        grid=(rows // TILE,),
        in_specs=[row, row, row, row, row, whole((3, width, width)), whole(vecs.shape)],
        out_specs=[row, acc, acc, acc, acc],
        out_shape=[jax.ShapeDtypeStruct((rows, width), F32), vec, vec, vec, vec],
        compiler_params=params(),
        cost_estimate=cost(6 * rows * width * width, 16 * rows * width),
        name="input_grad",
    )(x, dq, dk, dv, dr, ab, vecs)


def mask_terms(lengths, cells, context):
    usable = (jnp.arange(context) < lengths[0]) & (cells[0] == 1)
    bias = jnp.where(usable, 0.0, MASKED)
    kbias = jnp.broadcast_to(bias.astype(BF16)[:, None], (context, 128))
    rbias = bias[None, :]
    valid = jnp.broadcast_to(
        (jnp.arange(context) < lengths[0]).astype(F32)[:, None], (context, 128)
    )
    return kbias, rbias, valid


def gather_kernel(nz, n_small, own_ref, small_ref, ab_ref, c_ref, all_small_ref, send, recv, local):
    d = lax.axis_index("dp")
    f = lax.axis_index("fsdp")
    z, c = f // 2, f % 2
    half = own_ref.shape[2] // 2
    mate = z * 2 + (1 - c)
    flip_x = d + 1 - 2 * (d % 2)
    flip_y = lax.rem(d + 2, 4)
    flip_xy = lax.rem(flip_x + 2, 4)
    others = [lax.rem(z + k, nz) for k in range(1, nz)]

    barrier = pltpu.get_barrier_semaphore()
    partners = [(flip_x, f), (flip_y, f), (d, mate)]
    for o in others:
        partners += [(d, o * 2 + c), (d, o * 2 + 1 - c)]
    for p in partners:
        pl.semaphore_signal(barrier, inc=1, device_id=p, device_id_type=pl.DeviceIdType.MESH)
    pl.semaphore_wait(barrier, len(partners))

    def slot(g, block, shard):
        if g == 2:
            return c_ref.at[shard, block]
        return ab_ref.at[g * 4 + block, shard]

    count = [0]
    pending = []

    def copy(src, dst, device, last=True):
        s = count[0]
        count[0] += 1
        made = pltpu.make_async_remote_copy(
            src_ref=src, dst_ref=dst, send_sem=send.at[s], recv_sem=recv.at[s],
            device_id=device, device_id_type=pl.DeviceIdType.MESH,
        )
        made.start()
        if last:
            pending.append(made)
        return made

    def left(ref):
        return ref.at[:, 0:half]

    def right(ref):
        return ref.at[:, half : 2 * half]

    fetch = {}
    for o in others:
        copy(small_ref, all_small_ref.at[f], (d, o * 2 + c))
        copy(small_ref, all_small_ref.at[f], (d, o * 2 + 1 - c))
    copy(small_ref, all_small_ref.at[f], (d, mate))
    for g in range(3):
        for k, o in enumerate(others):
            fetch[g, k] = copy(own_ref.at[g * 4 + d], slot(g, d, f), (d, o * 2 + c), False)
    copy(own_ref.at[0:8], ab_ref.at[:, f], (d, mate))
    copy(own_ref.at[8:12], c_ref.at[f], (d, mate))
    keep = [
        pltpu.make_async_copy(own_ref.at[0:8], ab_ref.at[:, f], local.at[0]),
        pltpu.make_async_copy(own_ref.at[8:12], c_ref.at[f], local.at[1]),
        pltpu.make_async_copy(small_ref, all_small_ref.at[f], local.at[2]),
    ]
    for made in keep:
        made.start()
    arrived = list(fetch.values())

    units = [(g, k) for g in range(3) for k in range(nz - 1)]
    by_x, by_y, corner = {}, {}, {}
    for step in range(len(units) + 2):
        if step < len(units):
            g, k = units[step]
            shard = lax.rem(z + nz - 1 - k, nz) * 2 + c
            fetch[g, k].wait_recv()
            mine = slot(g, d, shard)
            by_x[step] = copy(mine, mine, (flip_x, f), False)
            by_y[step] = copy(mine, mine, (flip_y, f), False)
            copy(mine, mine, (d, mate))
        if 1 <= step <= len(units):
            g, k = units[step - 1]
            shard = lax.rem(z + nz - 1 - k, nz) * 2 + c
            by_x[step - 1].wait_recv()
            theirs = slot(g, flip_x, shard)
            first = copy(right(theirs), right(theirs), (flip_y, f), False)
            copy(theirs, theirs, (d, mate))
            by_y[step - 1].wait_recv()
            theirs = slot(g, flip_y, shard)
            second = copy(left(theirs), left(theirs), (flip_x, f), False)
            copy(theirs, theirs, (d, mate))
            corner[step - 1] = (first, second)
        if step >= 2:
            g, k = units[step - 2]
            shard = lax.rem(z + nz - 1 - k, nz) * 2 + c
            for made in corner[step - 2]:
                made.wait_recv()
            theirs = slot(g, flip_xy, shard)
            copy(theirs, theirs, (d, mate))
    arrived += list(by_x.values()) + list(by_y.values())
    arrived += [made for both in corner.values() for made in both]
    for made in arrived:
        made.wait_send()
    for made in pending:
        made.wait()
    for made in keep:
        made.wait()


def gather_copies(nz):
    return (2 * (nz - 1) + 1) + 3 * (nz - 1) + 2 + 3 * (nz - 1) * 8


def gather_weights(own, small, nz):
    r, width = own.shape[1:]
    copies = gather_copies(nz)
    any_spec = pl.BlockSpec(memory_space=pl.ANY)
    vmem = pl.BlockSpec(memory_space=pltpu.VMEM)
    return pl.pallas_call(
        partial(gather_kernel, nz, small.shape[0]),
        in_specs=[vmem, vmem],
        out_specs=[any_spec, any_spec, any_spec],
        out_shape=[
            jax.ShapeDtypeStruct((8, 2 * nz, r, width), BF16),
            jax.ShapeDtypeStruct((2 * nz, 4, r, width), BF16),
            jax.ShapeDtypeStruct((2 * nz,) + small.shape, BF16),
        ],
        scratch_shapes=[
            pltpu.SemaphoreType.DMA((copies,)),
            pltpu.SemaphoreType.DMA((copies,)),
            pltpu.SemaphoreType.DMA((3,)),
        ],
        compiler_params=pltpu.CompilerParams(
            collective_id=0, has_side_effects=True, vmem_limit_bytes=16 * 1024 * 1024
        ),
        name="gather_weights",
    )(own, small)


def core_split(res_ref, core, r, nz, send_ref, keep_ref):
    for i in range(nz):
        base = i * 2 * r
        send_ref[0, i] = res_ref[pl.ds(pl.multiple_of(base + (1 - core) * r, 8), r), :].astype(BF16)
        keep_ref[0, i] = res_ref[pl.ds(pl.multiple_of(base + core * r, 8), r), :].astype(BF16)


def grad_up_kernel(nz, r, ids_ref, a_ref, b_ref, send_ref, keep_ref, res_ref):
    res_ref[...] = mm_tn(a_ref[...], b_ref[...])
    core_split(res_ref, ids_ref[2], r, nz, send_ref, keep_ref)


def grad_up_split(ids, a, b, nz):
    rows, m = a.shape
    blocks = b.shape[1] // m
    r = m // (2 * nz)
    half = jax.ShapeDtypeStruct((blocks, nz, r, m), BF16)
    out = pl.BlockSpec((1, nz, r, m), lambda i, ids: (i, 0, 0, 0))
    return pl.pallas_call(
        partial(grad_up_kernel, nz, r),
        grid_spec=pltpu.PrefetchScalarGridSpec(
            num_scalar_prefetch=1,
            grid=(blocks,),
            in_specs=[
                pl.BlockSpec((rows, m), lambda i, ids: (0, 0), pipeline_mode=pl.Buffered(1)),
                pl.BlockSpec((rows, m), lambda i, ids: (0, i)),
            ],
            out_specs=[out, out],
            scratch_shapes=[pltpu.VMEM((m, m), F32)],
        ),
        out_shape=[half, half],
        compiler_params=params(),
        cost_estimate=cost(2 * rows * m * b.shape[1], 2 * (rows * m + rows * b.shape[1] + m * b.shape[1])),
        name="grad_up",
    )(ids, a, b)


def grad_attn_kernel(nz, r, ids_ref, a_ref, o_ref, q_ref, k_ref, v_ref, y_ref, send_ref, keep_ref, res_ref):
    step = pl.program_id(0)
    for i, (left, right) in enumerate(((a_ref, q_ref), (a_ref, k_ref), (a_ref, v_ref), (o_ref, y_ref))):
        @pl.when(step == i)
        def _():
            res_ref[...] = mm_tn(left[...], right[...])
    core_split(res_ref, ids_ref[2], r, nz, send_ref, keep_ref)


def grad_attn_split(ids, a1, o, dq, dk, dv, dy, nz):
    rows, m = a1.shape
    r = m // (2 * nz)
    half = jax.ShapeDtypeStruct((4, nz, r, m), BF16)
    out = pl.BlockSpec((1, nz, r, m), lambda i, ids: (i, 0, 0, 0))
    full = pl.BlockSpec((rows, m), lambda i, ids: (0, 0), pipeline_mode=pl.Buffered(1))
    return pl.pallas_call(
        partial(grad_attn_kernel, nz, r),
        grid_spec=pltpu.PrefetchScalarGridSpec(
            num_scalar_prefetch=1,
            grid=(4,),
            in_specs=[full] * 6,
            out_specs=[out, out],
            scratch_shapes=[pltpu.VMEM((m, m), F32)],
        ),
        out_shape=[half, half],
        compiler_params=params(),
        cost_estimate=cost(8 * rows * m * m, 2 * (6 * rows * m + 4 * m * m)),
        name="grad_attn",
    )(ids, a1, o, dq, dk, dv, dy)


def grad_down_kernel(r, ids_ref, a_ref, b_ref, send_ref, keep_ref, res_ref):
    res_ref[...] = mm_tn(a_ref[...], b_ref[...])
    core = ids_ref[2]
    for j in range(send_ref.shape[1]):
        for i in range(4):
            base = j * 8 * r + i * r
            there = pl.multiple_of(base + (1 - core) * 4 * r, 8)
            here = pl.multiple_of(base + core * 4 * r, 8)
            send_ref[i, j] = res_ref[pl.ds(there, r), :].astype(BF16)
            keep_ref[i, j] = res_ref[pl.ds(here, r), :].astype(BF16)


def grad_down_split(ids, a, b, nz):
    rows, hidden = a.shape
    n = b.shape[1]
    r = hidden // (8 * nz)
    per = hidden // 4
    half = jax.ShapeDtypeStruct((4, nz, r, n), BF16)
    out = pl.BlockSpec((4, nz // 4, r, n), lambda i, ids: (0, i, 0, 0))
    return pl.pallas_call(
        partial(grad_down_kernel, r),
        grid_spec=pltpu.PrefetchScalarGridSpec(
            num_scalar_prefetch=1,
            grid=(4,),
            in_specs=[
                pl.BlockSpec((rows, per), lambda i, ids: (0, i)),
                pl.BlockSpec((rows, n), lambda i, ids: (0, 0), pipeline_mode=pl.Buffered(1)),
            ],
            out_specs=[out, out],
            scratch_shapes=[pltpu.VMEM((per, n), F32)],
        ),
        out_shape=[half, half],
        compiler_params=params(),
        cost_estimate=cost(2 * rows * hidden * n, 2 * (rows * hidden + rows * n + hidden * n)),
        name="grad_down",
    )(ids, a, b)


def core_sum_kernel(n, ids_ref, *refs):
    d = ids_ref[0]
    flip_x = d + 1 - 2 * (d % 2)
    flip_y = lax.rem(d + 2, 4)
    flip_xy = lax.rem(flip_x + 2, 4)
    xs, ys, k0, k1 = refs[2 * n :]
    half = xs.shape[-1]
    lo, hi = slice(0, half), slice(half, 2 * half)
    for g in range(n):
        theirs, mine = refs[2 * g], refs[2 * g + 1]

        def total(block, cols):
            a = theirs[block, 0, :, cols].astype(F32)
            return (a + mine[block, 0, :, cols].astype(F32)).astype(BF16)

        xs[g, 0, 0] = total(flip_x, lo)
        xs[g, 1, 0] = total(flip_xy, lo)
        ys[g, 0, 0] = total(flip_y, hi)
        ys[g, 1, 0] = total(flip_xy, hi)
        k0[g, 0, 0] = total(d, lo)
        k0[g, 1, 0] = total(flip_y, lo)
        k1[g, 0, 0] = total(d, hi)
        k1[g, 1, 0] = total(flip_x, hi)


def core_sum(ids, pairs):
    n = len(pairs)
    blocks, nz, r, width = pairs[0][0].shape
    half = width // 2
    spec = pl.BlockSpec((4, 1, r, width), lambda i, ids: (0, i, 0, 0))
    out = pl.BlockSpec((n, 2, 1, r, half), lambda i, ids: (0, 0, i, 0, 0))
    shape = jax.ShapeDtypeStruct((n, 2, nz, r, half), BF16)
    size = 4 * nz * r * width * n
    return pl.pallas_call(
        partial(core_sum_kernel, n),
        grid_spec=pltpu.PrefetchScalarGridSpec(
            num_scalar_prefetch=1, grid=(nz,), in_specs=[spec] * (2 * n), out_specs=[out] * 4
        ),
        out_shape=[shape] * 4,
        compiler_params=params(),
        cost_estimate=cost(size, 6 * size),
        name="core_sum",
    )(ids, *[a for pair in pairs for a in pair])


def plane_one_kernel(xr, yr, k0, k1, xs, ys, keep0, keep1):
    ys[:, 0] = (k0[:, 1, 0].astype(F32) + xr[:, 1, 0].astype(F32)).astype(BF16)
    xs[:, 0] = (k1[:, 1, 0].astype(F32) + yr[:, 1, 0].astype(F32)).astype(BF16)
    keep0[:, 0] = (k0[:, 0, 0].astype(F32) + xr[:, 0, 0].astype(F32)).astype(BF16)
    keep1[:, 0] = (k1[:, 0, 0].astype(F32) + yr[:, 0, 0].astype(F32)).astype(BF16)


def plane_one(xr, yr, k0, k1):
    n, _, nz, r, half = xr.shape
    spec = pl.BlockSpec((n, 2, 1, r, half), lambda i: (0, 0, i, 0, 0))
    out = pl.BlockSpec((n, 1, r, half), lambda i: (0, i, 0, 0))
    size = 4 * n * nz * r * half
    return pl.pallas_call(
        plane_one_kernel,
        grid=(nz,),
        in_specs=[spec] * 4,
        out_specs=[out] * 4,
        out_shape=[jax.ShapeDtypeStruct((n, nz, r, half), BF16)] * 4,
        compiler_params=params(),
        cost_estimate=cost(size, 6 * size),
        name="plane_one",
    )(xr, yr, k0, k1)


def plane_two_kernel(nz, ids_ref, xr, yr, keep0, keep1, *outs):
    z = ids_ref[1]
    half = xr.shape[-1]
    for k in range(nz):
        at = lax.rem(z + k, nz)
        for g in range(xr.shape[0]):
            outs[k][g, :, 0:half] = (keep0[g, at].astype(F32) + yr[g, at].astype(F32)).astype(BF16)
            outs[k][g, :, half:] = (keep1[g, at].astype(F32) + xr[g, at].astype(F32)).astype(BF16)


def one_step(kernel, n_ids, operands, shapes, flops, name):
    vmem = pl.BlockSpec(memory_space=pltpu.VMEM)
    smem = pl.BlockSpec(memory_space=pltpu.SMEM)
    moved = sum(x.size * x.dtype.itemsize for x in operands[n_ids:])
    return pl.pallas_call(
        kernel,
        in_specs=[smem] * n_ids + [vmem] * (len(operands) - n_ids),
        out_specs=[vmem] * len(shapes),
        out_shape=shapes,
        compiler_params=pltpu.CompilerParams(vmem_limit_bytes=24 * 1024 * 1024),
        cost_estimate=cost(flops, 2 * moved),
        name=name,
    )(*operands)


def plane_two(ids, xr, yr, keep0, keep1):
    n, nz, r, half = xr.shape
    shape = jax.ShapeDtypeStruct((n, r, 2 * half), BF16)
    return one_step(
        partial(plane_two_kernel, nz), 1, (ids, xr, yr, keep0, keep1), [shape] * nz, 2 * xr.size, "plane_two"
    )


def outer_sum_kernel(*refs):
    acc = refs[0][...].astype(F32)
    for ref in refs[1:-1]:
        acc = acc + ref[...].astype(F32)
    refs[-1][...] = acc.astype(BF16)


def outer_sum(parts):
    shape = jax.ShapeDtypeStruct(parts[0].shape, BF16)
    return one_step(outer_sum_kernel, 0, parts, [shape], len(parts) * parts[0].size, "outer_sum")[0]


def place_mlp_kernel(ids_ref, *refs):
    up_ref, down_ref = refs[4:]
    width = up_ref.shape[1] // 4
    r = up_ref.shape[0]
    d = ids_ref[0]
    flip_x = d + 1 - 2 * (d % 2)
    flip_y = lax.rem(d + 2, 4)
    flip_xy = lax.rem(flip_x + 2, 4)
    for ref, block in zip(refs[:4], (d, flip_x, flip_y, flip_xy)):
        up_ref[:, pl.ds(pl.multiple_of(block * width, 128), width)] = ref[0].astype(F32)
        down_ref[pl.ds(pl.multiple_of(block * r, 8), r), :] = ref[1].astype(F32)


def place_attn_kernel(ids_ref, *refs):
    qkv_ref, out_ref = refs[4:]
    width = out_ref.shape[1]
    d = ids_ref[0]
    flip_x = d + 1 - 2 * (d % 2)
    flip_y = lax.rem(d + 2, 4)
    flip_xy = lax.rem(flip_x + 2, 4)
    for ref, block in zip(refs[:4], (d, flip_x, flip_y, flip_xy)):
        @pl.when(block < 3)
        def _():
            qkv_ref[:, pl.ds(pl.multiple_of(block * width, 128), width)] = ref[0].astype(F32)

        @pl.when(block == 3)
        def _():
            out_ref[...] = ref[0].astype(F32)


def swap_core(x, nf):
    return lax.ppermute(x, "fsdp", [(i, i ^ 1) for i in range(nf)])


def swap_dp(x, flip):
    return lax.ppermute(x, "dp", [(i, i ^ flip) for i in range(4)])


def shift_outer(x, k, nf):
    return lax.ppermute(x, "fsdp", [(i, (i + 2 * k) % nf) for i in range(nf)])


def reduce_groups(ids, halves, kernel, shapes, nf, name):
    nz = nf // 2
    pairs = [(swap_core(send, nf), keep) for send, keep in halves]
    xs, ys, k0, k1 = core_sum(ids, pairs)
    xs2, ys2, keep0, keep1 = None, None, None, None
    xr, yr = swap_dp(xs, 1), swap_dp(ys, 2)
    xs2_ys2 = plane_one(xr, yr, k0, k1)
    xs2, ys2, keep0, keep1 = xs2_ys2
    xr, yr = swap_dp(xs2, 1), swap_dp(ys2, 2)
    parts = plane_two(ids, xr, yr, keep0, keep1)
    terms = [parts[0]] + [shift_outer(parts[k], k, nf) for k in range(1, nz)]
    mine = outer_sum(tuple(terms))
    quarters = (mine, swap_dp(mine, 1), swap_dp(mine, 2), swap_dp(mine, 3))
    return one_step(kernel, 1, (ids,) + quarters, shapes, 4 * mine.size, name)


def sum_small(x, nf):
    x = x + swap_core(x, nf)
    x = x + swap_dp(x, 1)
    x = x + swap_dp(x, 2)
    total = x
    for k in range(1, nf // 2):
        total = total + shift_outer(x, k, nf)
    return total


def per_device(
    tokens, lengths, cells, cotangent, ln1_gain, ln1_bias, w_qkv, b_query, b_value, w_out, b_out,
    ln2_gain, ln2_bias, w_up, b_up, w_down, b_down,
):
    seqs, context, width = tokens.shape
    r = w_qkv.shape[0]
    nf = width // r
    nz = nf // 2
    f = lax.axis_index("fsdp")
    ids = jnp.stack([lax.axis_index("dp"), f // 2, f % 2]).astype(jnp.int32)
    vectors = (ln1_gain, ln1_bias, b_query, b_value, b_out, ln2_gain, ln2_bias, b_down, b_up)
    flat = jnp.concatenate(vectors)
    small_rows = -(-flat.shape[0] // 2048) * 16
    small = jnp.pad(flat, (0, small_rows * 128 - flat.shape[0])).reshape(small_rows, 128)
    own = jnp.stack(
        [w_qkv[:, i * width : (i + 1) * width] for i in range(3)]
        + [w_out]
        + [w_up[:, i * width : (i + 1) * width] for i in range(4)]
        + [w_down[i * r : (i + 1) * r] for i in range(4)]
    )
    ab, down_full, smalls = gather_weights(own, small, nz)
    ab = ab.reshape(8, width, width)
    down_full = down_full.reshape(4 * width, width)
    smalls = smalls.reshape(nf, -1).astype(F32)
    vecs = smalls[:, : 8 * r].reshape(nf, 8, r).transpose(1, 0, 2).reshape(8, width)
    bu = smalls[:, 8 * r : 12 * r].reshape(1, 4 * width)
    x = tokens[0]
    kbias, rbias, valid = mask_terms(lengths, cells, context)
    a1, qkv = qkv_forward(x, ab, vecs, 0.125)
    o, qa = attn_forward(qkv, kbias, rbias)
    out, dm, a2, g, du, dr, dy, do, s_g2, s_h2, s_bu, s_bd, s_bo = mlp_both(
        x, o, cotangent[0], valid, ab, down_full, vecs, bu
    )
    down_halves = grad_down_split(ids, g, dm, nz)
    up_halves = grad_up_split(ids, a2, du, nz)
    grad_up, grad_down = reduce_groups(
        ids, (up_halves, down_halves), place_mlp_kernel,
        [jax.ShapeDtypeStruct(w_up.shape, F32), jax.ShapeDtypeStruct(w_down.shape, F32)], nf, "place_mlp",
    )
    parts = [attn_backward(qa, qkv, o, do, kbias, p, 3) for p in (0, 3)]
    dq, dk, dv = (jnp.concatenate(both, axis=1) for both in zip(*parts))
    attn_halves = grad_attn_split(ids, a1, o, dq, dk, dv, dy, nz)
    grad_x, s_g1, s_h1, s_bq, s_bv = input_grad(x, dq, dk, dv, dr, ab, vecs)
    grad_qkv, grad_out = reduce_groups(
        ids, (attn_halves,), place_attn_kernel,
        [jax.ShapeDtypeStruct(w_qkv.shape, F32), jax.ShapeDtypeStruct(w_out.shape, F32)], nf, "place_attn",
    )
    sums = jnp.concatenate(
        [s.reshape(nf, -1) for s in (s_g1, s_h1, s_bq, s_bv, s_bo, s_g2, s_h2, s_bd, s_bu)], axis=1
    )
    sums = sum_small(sums.reshape(-1, 128), nf).reshape(nf, -1)
    mine = lax.dynamic_index_in_dim(sums, f, axis=0, keepdims=False)
    g_g1, g_h1, g_bq, g_bv, g_bo, g_g2, g_h2, g_bd = (mine[i * r : (i + 1) * r] for i in range(8))
    g_bu = mine[8 * r :]
    return (
        out[None], grad_x[None], g_g1, g_h1, grad_qkv, g_bq, g_bv, grad_out, g_bo, g_g2, g_h2,
        grad_up, g_bu, grad_down, g_bd,
    )


def solution(mesh):
    split = P(("dp", "fsdp"), None, None)
    vec, mat = P("fsdp"), P("fsdp", None)
    in_specs = (
        split, P(("dp", "fsdp")), P(("dp", "fsdp"), None), split,
        vec, vec, mat, vec, vec, mat, vec, vec, vec, mat, vec, mat, vec,
    )
    out_specs = (split, split, vec, vec, mat, vec, vec, mat, vec, vec, vec, mat, vec, mat, vec)
    return jax.shard_map(
        per_device, mesh=mesh, in_specs=in_specs, out_specs=out_specs, check_vma=False
    )
```

```python
from functools import partial
import math

import jax
import jax.numpy as jnp
from jax import lax
from jax.experimental import pallas as pl
from jax.experimental.pallas import tpu as pltpu
from jax.sharding import PartitionSpec as P

HEADS = 12
EPSILON = 1e-05
GELU_C = 0.7978845608028654
GELU_A = 0.044715
MASKED = -1e30
TILE = 256
VMEM_BYTES = 60 * 1024 * 1024
F32 = jnp.float32
BF16 = jnp.bfloat16


def mm(a, b):
    return jnp.dot(a, b, preferred_element_type=F32)


def mm_nt(a, b):
    return lax.dot_general(a, b, (((1,), (1,)), ((), ())), preferred_element_type=F32)


def mm_tn(a, b):
    return lax.dot_general(a, b, (((0,), (0,)), ((), ())), preferred_element_type=F32)


def params(**kw):
    return pltpu.CompilerParams(
        dimension_semantics=("arbitrary",), vmem_limit_bytes=VMEM_BYTES, **kw
    )


def cost(flops, bytes_accessed, transcendentals=0):
    return pl.CostEstimate(
        flops=int(flops), bytes_accessed=int(bytes_accessed), transcendentals=int(transcendentals)
    )


def norm_forward(values):
    row_mean = jnp.mean(values, axis=-1, keepdims=True)
    centered = values - row_mean
    inv_std = lax.rsqrt(jnp.mean(centered * centered, axis=-1, keepdims=True) + EPSILON)
    return centered * inv_std, inv_std


def norm_backward(grad_normed, normalized, inv_std, gain):
    scaled = grad_normed * gain
    return inv_std * (
        scaled
        - jnp.mean(scaled, axis=-1, keepdims=True)
        - normalized * jnp.mean(scaled * normalized, axis=-1, keepdims=True)
    )


def gelu_pair(u):
    square = u * u
    tanh_part = jnp.tanh(u * (GELU_C + (GELU_C * GELU_A) * square))
    half = 0.5 + 0.5 * tanh_part
    value = u * half
    slope = half + value * (1.0 - tanh_part) * (GELU_C + (3.0 * GELU_C * GELU_A) * square)
    return value, slope


def whole(shape):
    return pl.BlockSpec(shape, lambda i: (0,) * len(shape), pipeline_mode=pl.Buffered(1))


def rows_spec(tile, width):
    return pl.BlockSpec((tile, width), lambda i: (i, 0))


def qkv_kernel(scale, x_ref, w_ref, vec_ref, a1_ref, qkv_ref):
    width = x_ref.shape[1]
    gain, shift, bq, bv = (vec_ref[i : i + 1, :] for i in range(4))
    xhat, _ = norm_forward(x_ref[...].astype(F32))
    a1 = (xhat * gain + shift).astype(BF16)
    a1_ref[...] = a1
    q = mm(a1, w_ref[0])
    qkv_ref[:, 0:width] = ((q + bq) * scale).astype(BF16)
    k = mm(a1, w_ref[1])
    qkv_ref[:, width : 2 * width] = k.astype(BF16)
    v = mm(a1, w_ref[2])
    qkv_ref[:, 2 * width : 3 * width] = (v + bv).astype(BF16)


def qkv_forward(x, ab, vecs, scale):
    rows, width = x.shape
    return pl.pallas_call(
        partial(qkv_kernel, scale),
        grid=(rows // TILE,),
        in_specs=[rows_spec(TILE, width), whole((3, width, width)), whole(vecs.shape)],
        out_specs=[rows_spec(TILE, width), rows_spec(TILE, 3 * width)],
        out_shape=[
            jax.ShapeDtypeStruct((rows, width), BF16),
            jax.ShapeDtypeStruct((rows, 3 * width), BF16),
        ],
        compiler_params=params(),
        cost_estimate=cost(6 * rows * width * width, 12 * rows * width),
        name="qkv_forward",
    )(x, ab, vecs)


def split3(value):
    first = value.astype(BF16)
    rest = value - first.astype(F32)
    second = rest.astype(BF16)
    third = (rest - second.astype(F32)).astype(BF16)
    return first, second, third


def attn_fwd_kernel(q_ref, k_ref, v_ref, kbias_ref, rbias_ref, o_ref, qa_ref, mask_ref):
    blocks = q_ref.shape[0] // TILE
    lane = lax.broadcasted_iota(jnp.int32, (1, 128), 1)

    @pl.when(pl.program_id(0) == 0)
    def _():
        row = lax.broadcasted_iota(jnp.int32, (TILE, TILE), 0)
        col = lax.broadcasted_iota(jnp.int32, (TILE, TILE), 1)
        for i in range(blocks):
            usable = rbias_ref[:, i * TILE : (i + 1) * TILE]
            mask_ref[i] = jnp.where(row == col, 0.0, jnp.where(row > col, usable, MASKED))

    zero = jnp.zeros((), BF16)
    one = jnp.ones((), BF16)
    for head in range(2):
        base = 64 * head
        extra = 64 - base
        own = (lane >= base) & (lane < base + 64)
        k_off = jnp.where(own, k_ref[...], jnp.where(lane == extra, kbias_ref[...], zero))
        for i in range(blocks):
            here = slice(i * TILE, (i + 1) * TILE)
            q = jnp.where(own, q_ref[here, :], zero)
            q_off = jnp.where(lane == extra, one, q)
            s_diag = mm_nt(q, k_ref[here, :]) + mask_ref[i]
            row_max = jnp.max(s_diag, axis=-1, keepdims=True)
            if i:
                s_off = mm_nt(q_off, k_off[: i * TILE])
                row_max = jnp.maximum(row_max, jnp.max(s_off, axis=-1, keepdims=True))
            e_diag = jnp.exp(s_diag - row_max)
            total = jnp.sum(e_diag, axis=-1, keepdims=True)
            o = mm(e_diag.astype(BF16), v_ref[here, :])
            if i:
                e_off = jnp.exp(s_off - row_max)
                total += jnp.sum(e_off, axis=-1, keepdims=True)
                o += mm(e_off.astype(BF16), v_ref[0 : i * TILE, :])
            o = (o * (1.0 / total)).astype(BF16)
            if head:
                o_ref[here, :] = jnp.where(own, o, o_ref[here, :])
            else:
                o_ref[here, :] = o
            first, second, third = split3(-(row_max + jnp.log(total)))
            qa = jnp.where(lane == extra + 1, first, q_off)
            qa = jnp.where(lane == extra + 2, second, qa)
            qa = jnp.where(lane == extra + 3, third, qa)
            qa_ref[here, 128 * head : 128 * head + 128] = qa


def attn_forward(qkv, kbias, rbias):
    rows = qkv.shape[0]
    width = qkv.shape[1] // 3
    pairs = width // 128

    def part(p):
        return pl.BlockSpec((rows, 128), lambda i: (0, p * pairs + i))

    return pl.pallas_call(
        attn_fwd_kernel,
        grid=(pairs,),
        in_specs=[part(0), part(1), part(2), whole(kbias.shape), whole(rbias.shape)],
        out_specs=[part(0), pl.BlockSpec((rows, 256), lambda i: (0, i))],
        out_shape=[
            jax.ShapeDtypeStruct((rows, width), BF16),
            jax.ShapeDtypeStruct((rows, 2 * width), BF16),
        ],
        scratch_shapes=[pltpu.VMEM((rows // TILE, TILE, TILE), F32)],
        compiler_params=params(),
        cost_estimate=cost(8 * rows * rows * width, 12 * rows * width),
        name="attn_forward",
    )(qkv, qkv, qkv, kbias, rbias)


def attn_bwd_kernel(
    qa_ref, k_ref, v_ref, o_ref, do_ref, kbias_ref, dq_ref, dk_ref, dv_ref, mask_ref, doa_ref, dqt_ref,
    between=None,
):
    rows = k_ref.shape[0]
    blocks = rows // TILE
    lane = lax.broadcasted_iota(jnp.int32, (1, 128), 1)

    @pl.when(pl.program_id(0) == 0)
    def _():
        key = lax.broadcasted_iota(jnp.int32, (TILE, TILE), 0)
        query = lax.broadcasted_iota(jnp.int32, (TILE, TILE), 1)
        for i in range(blocks):
            usable = kbias_ref[i * TILE : (i + 1) * TILE, 0:1].astype(F32)
            mask_ref[i] = jnp.where(key == query, 0.0, jnp.where(query > key, usable, MASKED))

    zero = jnp.zeros((), BF16)
    one = jnp.ones((), BF16)
    product = do_ref[...].astype(F32) * o_ref[...].astype(F32)
    kt = k_ref[...].T
    for head in range(2):
        base = 64 * head
        extra = 64 - base
        own = (lane >= base) & (lane < base + 64)
        terms = (lane > extra) & (lane <= extra + 3)
        qa_cols = slice(128 * head, 128 * head + 128)
        if between is not None:
            between(head)
        inner = -jnp.sum(jnp.where(own, product, 0.0), axis=-1, keepdims=True)
        first, second, third = split3(inner)
        doa = jnp.where(own, do_ref[...], zero)
        doa = jnp.where(lane == extra + 1, first, doa)
        doa = jnp.where(lane == extra + 2, second, doa)
        doa_ref[...] = jnp.where(lane == extra + 3, third, doa)
        for j in range(blocks):
            here = slice(j * TILE, (j + 1) * TILE)
            after = slice((j + 1) * TILE, rows)
            k_diag = jnp.where(own, k_ref[here, :], jnp.where(terms, one, zero))
            v_aug = jnp.where(own, v_ref[here, :], jnp.where(terms, one, zero))
            p_diag = jnp.exp(mm_nt(k_diag, qa_ref[here, qa_cols]) + mask_ref[j])
            dp_diag = mm_nt(v_aug, doa_ref[here, :])
            ds_diag = (p_diag * dp_diag).astype(BF16)
            dv = mm(p_diag.astype(BF16), do_ref[here, :])
            dk = mm(ds_diag, qa_ref[here, qa_cols])
            dq_diag = mm(kt[:, here], ds_diag)
            if j:
                dqt_ref[:, here] += dq_diag
            else:
                dqt_ref[:, here] = dq_diag
            if j + 1 < blocks:
                k_off = jnp.where(lane == extra, kbias_ref[here, :], k_diag)
                p_off = jnp.exp(mm_nt(k_off, qa_ref[after, qa_cols]))
                dp_off = mm_nt(v_aug, doa_ref[after, :])
                ds_off = (p_off * dp_off).astype(BF16)
                dv += mm(p_off.astype(BF16), do_ref[after, :])
                dk += mm(ds_off, qa_ref[after, qa_cols])
                dq_off = mm(kt[:, here], ds_off)
                if j:
                    dqt_ref[:, after] += dq_off
                else:
                    dqt_ref[:, after] = dq_off
            dk = dk.astype(BF16)
            dv = dv.astype(BF16)
            if head:
                dk_ref[here, :] = jnp.where(own, dk, dk_ref[here, :])
                dv_ref[here, :] = jnp.where(own, dv, dv_ref[here, :])
            else:
                dk_ref[here, :] = dk
                dv_ref[here, :] = dv
        dq = (dqt_ref[...] * 0.125).astype(BF16).T
        if head:
            dq_ref[...] = jnp.where(own, dq, dq_ref[...])
        else:
            dq_ref[...] = dq


def attn_backward(qa, qkv, o, do, kbias, first_pair, pair_count):
    rows, width = o.shape
    pairs = width // 128

    def part(p):
        return pl.BlockSpec((rows, 128), lambda i: (0, p * pairs + first_pair + i))

    out = pl.BlockSpec((rows, 128), lambda i: (0, i))
    shape = jax.ShapeDtypeStruct((rows, 128 * pair_count), BF16)
    return pl.pallas_call(
        attn_bwd_kernel,
        grid=(pair_count,),
        in_specs=[
            pl.BlockSpec((rows, 256), lambda i: (0, first_pair + i)),
            part(1),
            part(2),
            part(0),
            part(0),
            whole(kbias.shape),
        ],
        out_specs=[out, out, out],
        out_shape=[shape, shape, shape],
        scratch_shapes=[
            pltpu.VMEM((rows // TILE, TILE, TILE), F32),
            pltpu.VMEM((rows, 128), BF16),
            pltpu.VMEM((128, rows), F32),
        ],
        compiler_params=params(),
        cost_estimate=cost(20 * rows * rows * 128 * pair_count, 18 * rows * 128 * pair_count),
        name="attn_backward",
    )(qa, qkv, qkv, o, do, kbias)


def mlp_kernel(
    x_ref, o_ref, cot_ref, valid_ref, wo_ref, wu_ref, wd_ref, vec_ref, bu_ref,
    out_ref, dm_ref, a2_ref, g_ref, du_ref, dr_ref, dy_ref, do_ref,
    s_gain_ref, s_shift_ref, s_bu_ref, s_bd_ref, s_bo_ref,
):
    chunk = wu_ref.shape[2]
    hidden = wd_ref.shape[0]
    bo, gain, shift, bd = (vec_ref[i : i + 1, :] for i in range(4, 8))
    middle = x_ref[...].astype(F32) + mm(o_ref[...], wo_ref[0]) + bo
    xhat, inv_std = norm_forward(middle)
    a2 = (xhat * gain + shift).astype(BF16)
    a2_ref[...] = a2
    dout = cot_ref[...].astype(F32) * valid_ref[:, 0:1]
    dm = dout.astype(BF16)
    dm_ref[...] = dm
    out = middle + bd
    da2 = jnp.zeros_like(middle)
    first = pl.program_id(0) == 0

    def add_sum(ref, cols, value):
        part = jnp.sum(value, axis=0, keepdims=True)
        ref[:, cols] = jnp.where(first, part, ref[:, cols] + part)

    for c in range(hidden // chunk):
        cols = slice(c * chunk, (c + 1) * chunk)
        u = mm(a2, wu_ref[c]) + bu_ref[:, cols]
        value, slope = gelu_pair(u)
        g = value.astype(BF16)
        g_ref[:, cols] = g
        out += mm(g, wd_ref[cols, :])
        du = (mm_nt(dm, wd_ref[cols, :]) * slope).astype(BF16)
        du_ref[:, cols] = du
        add_sum(s_bu_ref, cols, du.astype(F32))
        da2 += mm_nt(du, wu_ref[c])
    out_ref[...] = out.astype(BF16)
    every = slice(None)
    add_sum(s_bd_ref, every, dm.astype(F32))
    add_sum(s_gain_ref, every, da2 * xhat)
    add_sum(s_shift_ref, every, da2)
    dr = dout + norm_backward(da2, xhat, inv_std, gain)
    dr_ref[...] = dr
    dy = dr.astype(BF16)
    dy_ref[...] = dy
    add_sum(s_bo_ref, every, dy.astype(F32))
    do_ref[...] = mm_nt(dy, wo_ref[0]).astype(BF16)


def mlp_both(x, o, cot, valid, ab, w_down, vecs, b_up):
    rows, width = x.shape
    hidden = w_down.shape[0]
    row = rows_spec(TILE, width)
    wide = rows_spec(TILE, hidden)
    acc = pl.BlockSpec((1, width), lambda i: (0, 0))
    acc_wide = pl.BlockSpec((1, hidden), lambda i: (0, 0))

    def shape(r, c, t):
        return jax.ShapeDtypeStruct((r, c), t)

    return pl.pallas_call(
        mlp_kernel,
        grid=(rows // TILE,),
        in_specs=[
            row, row, row, rows_spec(TILE, 128),
            pl.BlockSpec((1, width, width), lambda i: (3, 0, 0), pipeline_mode=pl.Buffered(1)),
            pl.BlockSpec((4, width, width), lambda i: (1, 0, 0), pipeline_mode=pl.Buffered(1)),
            whole(w_down.shape), whole(vecs.shape), whole(b_up.shape),
        ],
        out_specs=[row, row, row, wide, wide, row, row, row, acc, acc, acc_wide, acc, acc],
        out_shape=[
            shape(rows, width, BF16), shape(rows, width, BF16), shape(rows, width, BF16),
            shape(rows, hidden, BF16), shape(rows, hidden, BF16), shape(rows, width, F32),
            shape(rows, width, BF16), shape(rows, width, BF16),
            shape(1, width, F32), shape(1, width, F32), shape(1, hidden, F32),
            shape(1, width, F32), shape(1, width, F32),
        ],
        compiler_params=params(),
        cost_estimate=cost(rows * width * (8 * hidden + 4 * width), 24 * rows * width + 12 * rows * hidden),
        name="mlp_both",
    )(x, o, cot, valid, ab, ab, w_down, vecs, b_up)


def input_kernel(
    x_ref, dq_ref, dk_ref, dv_ref, dr_ref, w_ref, vec_ref, out_ref, s_gain_ref, s_shift_ref, s_bq_ref, s_bv_ref
):
    width = x_ref.shape[1]
    xhat, inv_std = norm_forward(x_ref[...].astype(F32))
    da = mm_nt(dq_ref[...], w_ref[0])
    da += mm_nt(dk_ref[...], w_ref[1])
    da += mm_nt(dv_ref[...], w_ref[2])
    first = pl.program_id(0) == 0

    def add_sum(ref, value):
        part = jnp.sum(value, axis=0, keepdims=True)
        ref[...] = jnp.where(first, part, ref[...] + part)

    add_sum(s_gain_ref, da * xhat)
    add_sum(s_shift_ref, da)
    add_sum(s_bq_ref, dq_ref[...].astype(F32))
    add_sum(s_bv_ref, dv_ref[...].astype(F32))
    out_ref[...] = dr_ref[...] + norm_backward(da, xhat, inv_std, vec_ref[0:1, :])


def input_grad(x, dq, dk, dv, dr, ab, vecs):
    rows, width = x.shape
    row = rows_spec(TILE, width)
    acc = pl.BlockSpec((1, width), lambda i: (0, 0))
    vec = jax.ShapeDtypeStruct((1, width), F32)
    return pl.pallas_call(
        input_kernel,
        grid=(rows // TILE,),
        in_specs=[row, row, row, row, row, whole((3, width, width)), whole(vecs.shape)],
        out_specs=[row, acc, acc, acc, acc],
        out_shape=[jax.ShapeDtypeStruct((rows, width), F32), vec, vec, vec, vec],
        compiler_params=params(),
        cost_estimate=cost(6 * rows * width * width, 16 * rows * width),
        name="input_grad",
    )(x, dq, dk, dv, dr, ab, vecs)


def mask_terms(lengths, cells, context):
    usable = (jnp.arange(context) < lengths[0]) & (cells[0] == 1)
    bias = jnp.where(usable, 0.0, MASKED)
    kbias = jnp.broadcast_to(bias.astype(BF16)[:, None], (context, 128))
    rbias = bias[None, :]
    valid = jnp.broadcast_to(
        (jnp.arange(context) < lengths[0]).astype(F32)[:, None], (context, 128)
    )
    return kbias, rbias, valid


def gather_kernel(nz, n_small, own_ref, small_ref, ab_ref, c_ref, all_small_ref, send, recv, local):
    d = lax.axis_index("dp")
    f = lax.axis_index("fsdp")
    z, c = f // 2, f % 2
    half = own_ref.shape[2] // 2
    mate = z * 2 + (1 - c)
    flip_x = d + 1 - 2 * (d % 2)
    flip_y = lax.rem(d + 2, 4)
    flip_xy = lax.rem(flip_x + 2, 4)
    others = [lax.rem(z + k, nz) for k in range(1, nz)]

    barrier = pltpu.get_barrier_semaphore()
    partners = [(flip_x, f), (flip_y, f), (d, mate)]
    for o in others:
        partners += [(d, o * 2 + c), (d, o * 2 + 1 - c)]
    for p in partners:
        pl.semaphore_signal(barrier, inc=1, device_id=p, device_id_type=pl.DeviceIdType.MESH)
    pl.semaphore_wait(barrier, len(partners))

    def slot(g, block, shard):
        if g == 2:
            return c_ref.at[shard, block]
        return ab_ref.at[g * 4 + block, shard]

    count = [0]
    pending = []

    def copy(src, dst, device, last=True):
        s = count[0]
        count[0] += 1
        made = pltpu.make_async_remote_copy(
            src_ref=src, dst_ref=dst, send_sem=send.at[s], recv_sem=recv.at[s],
            device_id=device, device_id_type=pl.DeviceIdType.MESH,
        )
        made.start()
        if last:
            pending.append(made)
        return made

    def left(ref):
        return ref.at[:, 0:half]

    def right(ref):
        return ref.at[:, half : 2 * half]

    fetch = {}
    for o in others:
        copy(small_ref, all_small_ref.at[f], (d, o * 2 + c))
        copy(small_ref, all_small_ref.at[f], (d, o * 2 + 1 - c))
    copy(small_ref, all_small_ref.at[f], (d, mate))
    for g in range(3):
        for k, o in enumerate(others):
            fetch[g, k] = copy(own_ref.at[g * 4 + d], slot(g, d, f), (d, o * 2 + c), False)
    copy(own_ref.at[0:8], ab_ref.at[:, f], (d, mate))
    copy(own_ref.at[8:12], c_ref.at[f], (d, mate))
    keep = [
        pltpu.make_async_copy(own_ref.at[0:8], ab_ref.at[:, f], local.at[0]),
        pltpu.make_async_copy(own_ref.at[8:12], c_ref.at[f], local.at[1]),
        pltpu.make_async_copy(small_ref, all_small_ref.at[f], local.at[2]),
    ]
    for made in keep:
        made.start()
    arrived = list(fetch.values())

    units = [(g, k) for g in range(3) for k in range(nz - 1)]
    by_x, by_y, corner = {}, {}, {}
    for step in range(len(units) + 2):
        if step < len(units):
            g, k = units[step]
            shard = lax.rem(z + nz - 1 - k, nz) * 2 + c
            fetch[g, k].wait_recv()
            mine = slot(g, d, shard)
            by_x[step] = copy(mine, mine, (flip_x, f), False)
            by_y[step] = copy(mine, mine, (flip_y, f), False)
            copy(mine, mine, (d, mate))
        if 1 <= step <= len(units):
            g, k = units[step - 1]
            shard = lax.rem(z + nz - 1 - k, nz) * 2 + c
            by_x[step - 1].wait_recv()
            theirs = slot(g, flip_x, shard)
            first = copy(right(theirs), right(theirs), (flip_y, f), False)
            copy(theirs, theirs, (d, mate))
            by_y[step - 1].wait_recv()
            theirs = slot(g, flip_y, shard)
            second = copy(left(theirs), left(theirs), (flip_x, f), False)
            copy(theirs, theirs, (d, mate))
            corner[step - 1] = (first, second)
        if step >= 2:
            g, k = units[step - 2]
            shard = lax.rem(z + nz - 1 - k, nz) * 2 + c
            for made in corner[step - 2]:
                made.wait_recv()
            theirs = slot(g, flip_xy, shard)
            copy(theirs, theirs, (d, mate))
    arrived += list(by_x.values()) + list(by_y.values())
    arrived += [made for both in corner.values() for made in both]
    for made in arrived:
        made.wait_send()
    for made in pending:
        made.wait()
    for made in keep:
        made.wait()


def gather_copies(nz):
    return (2 * (nz - 1) + 1) + 3 * (nz - 1) + 2 + 3 * (nz - 1) * 8


def gather_weights(own, small, nz):
    r, width = own.shape[1:]
    copies = gather_copies(nz)
    any_spec = pl.BlockSpec(memory_space=pl.ANY)
    vmem = pl.BlockSpec(memory_space=pltpu.VMEM)
    return pl.pallas_call(
        partial(gather_kernel, nz, small.shape[0]),
        in_specs=[vmem, vmem],
        out_specs=[any_spec, any_spec, any_spec],
        out_shape=[
            jax.ShapeDtypeStruct((8, 2 * nz, r, width), BF16),
            jax.ShapeDtypeStruct((2 * nz, 4, r, width), BF16),
            jax.ShapeDtypeStruct((2 * nz,) + small.shape, BF16),
        ],
        scratch_shapes=[
            pltpu.SemaphoreType.DMA((copies,)),
            pltpu.SemaphoreType.DMA((copies,)),
            pltpu.SemaphoreType.DMA((3,)),
        ],
        compiler_params=pltpu.CompilerParams(
            collective_id=0, has_side_effects=True, vmem_limit_bytes=16 * 1024 * 1024
        ),
        name="gather_weights",
    )(own, small)


def core_split(res_ref, core, r, nz, send_ref, keep_ref):
    for i in range(nz):
        base = i * 2 * r
        send_ref[0, i] = res_ref[pl.ds(pl.multiple_of(base + (1 - core) * r, 8), r), :].astype(BF16)
        keep_ref[0, i] = res_ref[pl.ds(pl.multiple_of(base + core * r, 8), r), :].astype(BF16)


def grad_up_kernel(nz, r, ids_ref, a_ref, b_ref, send_ref, keep_ref, res_ref):
    res_ref[...] = mm_tn(a_ref[...], b_ref[...])
    core_split(res_ref, ids_ref[2], r, nz, send_ref, keep_ref)


def grad_up_split(ids, a, b, nz):
    rows, m = a.shape
    blocks = b.shape[1] // m
    r = m // (2 * nz)
    half = jax.ShapeDtypeStruct((blocks, nz, r, m), BF16)
    out = pl.BlockSpec((1, nz, r, m), lambda i, ids: (i, 0, 0, 0))
    return pl.pallas_call(
        partial(grad_up_kernel, nz, r),
        grid_spec=pltpu.PrefetchScalarGridSpec(
            num_scalar_prefetch=1,
            grid=(blocks,),
            in_specs=[
                pl.BlockSpec((rows, m), lambda i, ids: (0, 0), pipeline_mode=pl.Buffered(1)),
                pl.BlockSpec((rows, m), lambda i, ids: (0, i)),
            ],
            out_specs=[out, out],
            scratch_shapes=[pltpu.VMEM((m, m), F32)],
        ),
        out_shape=[half, half],
        compiler_params=params(),
        cost_estimate=cost(2 * rows * m * b.shape[1], 2 * (rows * m + rows * b.shape[1] + m * b.shape[1])),
        name="grad_up",
    )(ids, a, b)


def grad_attn_kernel(nz, r, ids_ref, a_ref, o_ref, q_ref, k_ref, v_ref, y_ref, send_ref, keep_ref, res_ref):
    step = pl.program_id(0)
    for i, (left, right) in enumerate(((a_ref, q_ref), (a_ref, k_ref), (a_ref, v_ref), (o_ref, y_ref))):
        @pl.when(step == i)
        def _():
            res_ref[...] = mm_tn(left[...], right[...])
    core_split(res_ref, ids_ref[2], r, nz, send_ref, keep_ref)


def grad_attn_split(ids, a1, o, dq, dk, dv, dy, nz):
    rows, m = a1.shape
    r = m // (2 * nz)
    half = jax.ShapeDtypeStruct((4, nz, r, m), BF16)
    out = pl.BlockSpec((1, nz, r, m), lambda i, ids: (i, 0, 0, 0))
    full = pl.BlockSpec((rows, m), lambda i, ids: (0, 0), pipeline_mode=pl.Buffered(1))
    return pl.pallas_call(
        partial(grad_attn_kernel, nz, r),
        grid_spec=pltpu.PrefetchScalarGridSpec(
            num_scalar_prefetch=1,
            grid=(4,),
            in_specs=[full] * 6,
            out_specs=[out, out],
            scratch_shapes=[pltpu.VMEM((m, m), F32)],
        ),
        out_shape=[half, half],
        compiler_params=params(),
        cost_estimate=cost(8 * rows * m * m, 2 * (6 * rows * m + 4 * m * m)),
        name="grad_attn",
    )(ids, a1, o, dq, dk, dv, dy)


def grad_down_kernel(r, ids_ref, a_ref, b_ref, send_ref, keep_ref, res_ref):
    res_ref[...] = mm_tn(a_ref[...], b_ref[...])
    core = ids_ref[2]
    for j in range(send_ref.shape[1]):
        for i in range(4):
            base = j * 8 * r + i * r
            there = pl.multiple_of(base + (1 - core) * 4 * r, 8)
            here = pl.multiple_of(base + core * 4 * r, 8)
            send_ref[i, j] = res_ref[pl.ds(there, r), :].astype(BF16)
            keep_ref[i, j] = res_ref[pl.ds(here, r), :].astype(BF16)


def grad_down_split(ids, a, b, nz):
    rows, hidden = a.shape
    n = b.shape[1]
    r = hidden // (8 * nz)
    per = hidden // 4
    half = jax.ShapeDtypeStruct((4, nz, r, n), BF16)
    out = pl.BlockSpec((4, nz // 4, r, n), lambda i, ids: (0, i, 0, 0))
    return pl.pallas_call(
        partial(grad_down_kernel, r),
        grid_spec=pltpu.PrefetchScalarGridSpec(
            num_scalar_prefetch=1,
            grid=(4,),
            in_specs=[
                pl.BlockSpec((rows, per), lambda i, ids: (0, i)),
                pl.BlockSpec((rows, n), lambda i, ids: (0, 0), pipeline_mode=pl.Buffered(1)),
            ],
            out_specs=[out, out],
            scratch_shapes=[pltpu.VMEM((per, n), F32)],
        ),
        out_shape=[half, half],
        compiler_params=params(),
        cost_estimate=cost(2 * rows * hidden * n, 2 * (rows * hidden + rows * n + hidden * n)),
        name="grad_down",
    )(ids, a, b)


class Exchange:
    def __init__(self, sends, keeps, mine, core_in, x_in, y_in, x2_in, y2_in, z_in, owned, dp_in, sems):
        self.sends, self.keeps = sends, keeps
        self.mine, self.core_in = mine, core_in
        self.x_in, self.y_in, self.x2_in, self.y2_in = x_in, y_in, x2_in, y2_in
        self.z_in, self.owned, self.dp_in = z_in, owned, dp_in
        self.send_sem, self.recv_sem, self.load_sem = sems
        self.groups = len(sends)
        self.nz = mine.shape[0] // self.groups
        self.half = mine.shape[3] // 2
        self.units = self.groups * self.nz
        d = lax.axis_index("dp")
        f = lax.axis_index("fsdp")
        self.d, self.f, self.z, self.c = d, f, f // 2, f % 2
        self.x = d + 1 - 2 * (d % 2)
        self.y = lax.rem(d + 2, 4)
        self.xy = lax.rem(self.x + 2, 4)
        self.mate = self.z * 2 + 1 - self.c

    def barrier(self):
        barrier = pltpu.get_barrier_semaphore()
        partners = [(self.d, self.mate)] + [(p, self.f) for p in (self.x, self.y, self.xy)]
        partners += [(self.d, lax.rem(self.z + k, self.nz) * 2 + self.c) for k in range(1, self.nz)]
        for p in partners:
            pl.semaphore_signal(barrier, inc=1, device_id=p, device_id_type=pl.DeviceIdType.MESH)
        pl.semaphore_wait(barrier, len(partners))

    def remote(self, src, dst, index, device):
        return pltpu.make_async_remote_copy(
            src_ref=src, dst_ref=dst, send_sem=self.send_sem.at[index], recv_sem=self.recv_sem.at[index],
            device_id=device, device_id_type=pl.DeviceIdType.MESH,
        )

    def owner(self, u):
        return lax.rem(self.z + 1 + u % self.nz, self.nz)

    def core_copy(self, u):
        src = self.sends[u // self.nz].at[:, self.owner(u)]
        return self.remote(src, self.core_in.at[u], u * 8, (self.d, self.mate))

    def load(self, u):
        src = self.keeps[u // self.nz].at[:, self.owner(u)]
        return pltpu.make_async_copy(src, self.mine.at[u], self.load_sem.at[u])

    def plane_copies(self, u):
        lo, hi = slice(0, self.half), slice(self.half, 2 * self.half)
        m = self.mine.at[u]
        to_x, to_y = (self.x, self.f), (self.y, self.f)
        return [
            self.remote(m.at[self.x, :, lo], self.x_in.at[u, 0], u * 8 + 1, to_x),
            self.remote(m.at[self.y, :, hi], self.y_in.at[u, 0], u * 8 + 2, to_y),
            self.remote(m.at[self.xy, :, lo], self.x_in.at[u, 1], u * 8 + 3, to_x),
            self.remote(m.at[self.xy, :, hi], self.y_in.at[u, 1], u * 8 + 4, to_y),
        ]

    def second_copies(self, u):
        lo, hi = slice(0, self.half), slice(self.half, 2 * self.half)
        m = self.mine.at[u]
        return [
            self.remote(m.at[self.y, :, lo], self.y2_in.at[u], u * 8 + 5, (self.y, self.f)),
            self.remote(m.at[self.x, :, hi], self.x2_in.at[u], u * 8 + 6, (self.x, self.f)),
        ]

    def owner_copy(self, u):
        g, j = u // self.nz, u % self.nz
        return self.remote(
            self.mine.at[u, self.d], self.z_in.at[g, j], u * 8 + 7, (self.d, self.owner(u) * 2 + self.c)
        )

    def dp_copies(self, g):
        base = self.units * 8 + 3 * g
        return [
            self.remote(self.owned.at[g], self.dp_in.at[g, i], base + i, (p, self.f))
            for i, p in enumerate((self.x, self.y, self.xy))
        ]

    def start(self):
        for u in range(self.units):
            self.core_copy(u).start()
        for u in range(self.units):
            self.load(u).start()

    def add(self, u, block, cols, term):
        value = self.mine[u, block, :, cols].astype(F32) + term.astype(F32)
        self.mine[u, block, :, cols] = value.astype(BF16)

    def stage_one(self, u):
        self.load(u).wait()
        self.core_copy(u).wait_recv()
        for block in range(4):
            self.add(u, block, slice(None), self.core_in[u, block])
        for made in self.plane_copies(u):
            made.start()

    def stage_two(self, u):
        lo, hi = slice(0, self.half), slice(self.half, 2 * self.half)
        copies = self.plane_copies(u)
        copies[0].wait_recv()
        self.add(u, self.d, lo, self.x_in[u, 0])
        copies[1].wait_recv()
        self.add(u, self.d, hi, self.y_in[u, 0])
        copies[2].wait_recv()
        self.add(u, self.y, lo, self.x_in[u, 1])
        copies[3].wait_recv()
        self.add(u, self.x, hi, self.y_in[u, 1])
        for made in self.second_copies(u):
            made.start()

    def stage_three(self, u):
        lo, hi = slice(0, self.half), slice(self.half, 2 * self.half)
        copies = self.second_copies(u)
        copies[0].wait_recv()
        self.add(u, self.d, lo, self.y2_in[u])
        copies[1].wait_recv()
        self.add(u, self.d, hi, self.x2_in[u])
        if u % self.nz != self.nz - 1:
            self.owner_copy(u).start()

    def stage_four(self, g):
        last = g * self.nz + self.nz - 1
        total = self.mine[last, self.d].astype(F32)
        for j in range(self.nz - 1):
            self.owner_copy(g * self.nz + j).wait_recv()
            total = total + self.z_in[g, j].astype(F32)
        self.owned[g] = total.astype(BF16)
        for made in self.dp_copies(g):
            made.start()

    def blocks(self, g):
        yield self.d, self.owned[g].astype(F32)
        for i, (made, p) in enumerate(zip(self.dp_copies(g), (self.x, self.y, self.xy))):
            made.wait_recv()
            yield p, self.dp_in[g, i].astype(F32)

    def finish(self):
        for u in range(self.units):
            self.core_copy(u).wait_send()
            for made in self.plane_copies(u) + self.second_copies(u):
                made.wait_send()
            if u % self.nz != self.nz - 1:
                self.owner_copy(u).wait_send()
        for g in range(self.groups):
            for made in self.dp_copies(g):
                made.wait_send()

    def steps(self):
        return self.units + 2

    def step(self, t):
        if t < self.units:
            self.stage_one(t)
        if 1 <= t <= self.units:
            self.stage_two(t - 1)
        if 2 <= t:
            self.stage_three(t - 2)


def exchange_scratch(groups, nz, r, width, extra=0):
    units = groups * nz
    half = width // 2
    copies = units * 8 + 3 * groups + extra
    return [
        pltpu.VMEM((units, 4, r, width), BF16),
        pltpu.VMEM((units, 4, r, width), BF16),
        pltpu.VMEM((units, 2, r, half), BF16),
        pltpu.VMEM((units, 2, r, half), BF16),
        pltpu.VMEM((units, r, half), BF16),
        pltpu.VMEM((units, r, half), BF16),
        pltpu.VMEM((groups, nz - 1, r, width), BF16),
        pltpu.VMEM((groups, r, width), BF16),
        pltpu.VMEM((groups, 3, r, width), BF16),
        pltpu.SemaphoreType.DMA((copies,)),
        pltpu.SemaphoreType.DMA((copies,)),
        pltpu.SemaphoreType.DMA((units,)),
    ]


def attn_bwd_exchange_kernel(
    qa_ref, k_ref, v_ref, o_ref, do_ref, kbias_ref, up_send, up_keep, down_send, down_keep,
    dq_ref, dk_ref, dv_ref, up_ref, down_ref, mask_ref, doa_ref, dqt_ref, *scratch,
):
    ex = Exchange((down_send, up_send), (down_keep, up_keep), *scratch[:9], scratch[9:])
    pid = pl.program_id(0)
    grid = 6
    slots = 2 * grid - 1

    @pl.when(pid == 0)
    def _():
        ex.barrier()
        ex.start()

    plan = {}
    total = ex.steps()
    for t in range(total):
        plan.setdefault(1 + t * min(slots, total) // total, []).append(t)

    def between(half):
        for slot, todo in plan.items():
            if slot % 2 == half:
                @pl.when(pid == slot // 2)
                def _():
                    for t in todo:
                        ex.step(t)

    attn_bwd_kernel(
        qa_ref, k_ref, v_ref, o_ref, do_ref, kbias_ref, dq_ref, dk_ref, dv_ref, mask_ref, doa_ref, dqt_ref,
        between=between,
    )

    @pl.when(pid == grid - 1)
    def _():
        r = down_send.shape[2]
        width = down_send.shape[3]
        ex.stage_four(0)
        ex.stage_four(1)
        for block, value in ex.blocks(0):
            down_ref[pl.ds(pl.multiple_of(block * r, 8), r), :] = value
        for block, value in ex.blocks(1):
            up_ref[:, pl.ds(pl.multiple_of(block * width, 128), width)] = value
        ex.finish()


def attn_backward_exchange(qa, qkv, o, do, kbias, up_halves, down_halves, nz):
    rows, width = o.shape
    pairs = width // 128
    r = up_halves[0].shape[2]

    def part(p):
        return pl.BlockSpec((rows, 128), lambda i: (0, p * pairs + i))

    any_spec = pl.BlockSpec(memory_space=pl.ANY)
    out = pl.BlockSpec((rows, 128), lambda i: (0, i))
    shape = jax.ShapeDtypeStruct((rows, width), BF16)
    return pl.pallas_call(
        attn_bwd_exchange_kernel,
        grid=(pairs,),
        in_specs=[
            pl.BlockSpec((rows, 256), lambda i: (0, i)), part(1), part(2), part(0), part(0),
            whole(kbias.shape), any_spec, any_spec, any_spec, any_spec,
        ],
        out_specs=[out, out, out, whole((r, 4 * width)), whole((4 * r, width))],
        out_shape=[
            shape, shape, shape,
            jax.ShapeDtypeStruct((r, 4 * width), F32), jax.ShapeDtypeStruct((4 * r, width), F32),
        ],
        scratch_shapes=[
            pltpu.VMEM((rows // TILE, TILE, TILE), F32),
            pltpu.VMEM((rows, 128), BF16),
            pltpu.VMEM((128, rows), F32),
        ] + exchange_scratch(2, nz, r, width),
        compiler_params=params(collective_id=1, has_side_effects=True),
        cost_estimate=cost(20 * rows * rows * width, 18 * rows * width),
        name="attn_backward_exchange",
    )(qa, qkv, qkv, o, do, kbias, *up_halves, *down_halves)


def input_exchange_kernel(
    x_ref, dq_ref, dk_ref, dv_ref, dr_ref, w_ref, vec_ref, s_bo_ref, s_g2_ref, s_h2_ref, s_bd_ref, s_bu_ref,
    send_ref, keep_ref, out_ref, qkv_ref, wo_ref, sums_ref, small_in, *scratch,
):
    ex = Exchange((send_ref,), (keep_ref,), *scratch[:9], scratch[9:])
    pid = pl.program_id(0)
    steps = 4
    width = x_ref.shape[1]

    @pl.when(pid == 0)
    def _():
        ex.barrier()
        ex.start()
        sums_ref[...] = jnp.zeros_like(sums_ref)
        for i, ref in enumerate((s_bo_ref, s_g2_ref, s_h2_ref, s_bd_ref)):
            sums_ref[4 + i : 5 + i, :] = ref[...]
        for i in range(4):
            sums_ref[8 + i : 9 + i, :] = s_bu_ref[:, i * width : (i + 1) * width]

    xhat, inv_std = norm_forward(x_ref[...].astype(F32))
    da = mm_nt(dq_ref[...], w_ref[0])
    da += mm_nt(dk_ref[...], w_ref[1])
    da += mm_nt(dv_ref[...], w_ref[2])
    totals = (da * xhat, da, dq_ref[...].astype(F32), dv_ref[...].astype(F32))
    for i, value in enumerate(totals):
        sums_ref[i : i + 1, :] += jnp.sum(value, axis=0, keepdims=True)
    out_ref[...] = dr_ref[...] + norm_backward(da, xhat, inv_std, vec_ref[0:1, :])

    total = ex.steps()
    for slot in range(steps):
        todo = [t for t in range(total) if min(t * steps // ex.units, steps - 1) == slot]

        @pl.when(pid == slot)
        def _():
            for t in todo:
                ex.step(t)

    @pl.when(pid == steps - 1)
    def _():
        base = ex.units * 8 + 3
        hops = [(ex.d, ex.mate), (ex.x, ex.f), (ex.y, ex.f)]
        small = []

        def begin(i, device):
            made = ex.remote(sums_ref, small_in.at[i], base + i, device)
            made.start()
            small.append(made)

        begin(0, hops[0])
        ex.stage_four(0)
        for i in range(3):
            small[i].wait()
            sums_ref[...] += small_in[i]
            if i < 2:
                begin(i + 1, hops[i + 1])
        for k in range(1, ex.nz):
            begin(2 + k, (ex.d, lax.rem(ex.z + k, ex.nz) * 2 + ex.c))
        for block, value in ex.blocks(0):
            @pl.when(block < 3)
            def _():
                qkv_ref[:, pl.ds(pl.multiple_of(block * width, 128), width)] = value

            @pl.when(block == 3)
            def _():
                wo_ref[...] = value
        for made in small[3:]:
            made.wait()
        total_small = sums_ref[...]
        for k in range(1, ex.nz):
            total_small = total_small + small_in[2 + k]
        sums_ref[...] = total_small
        ex.finish()


def input_grad_exchange(x, dq, dk, dv, dr, ab, vecs, smalls, halves, nz):
    rows, width = x.shape
    tile = rows // 4
    r = halves[0].shape[2]
    row = rows_spec(tile, width)
    any_spec = pl.BlockSpec(memory_space=pl.ANY)
    return pl.pallas_call(
        input_exchange_kernel,
        grid=(4,),
        in_specs=[row, row, row, row, row, whole((3, width, width)), whole(vecs.shape)]
        + [whole(s.shape) for s in smalls] + [any_spec, any_spec],
        out_specs=[row, whole((r, 3 * width)), whole((r, width)), whole((16, width))],
        out_shape=[
            jax.ShapeDtypeStruct((rows, width), F32), jax.ShapeDtypeStruct((r, 3 * width), F32),
            jax.ShapeDtypeStruct((r, width), F32), jax.ShapeDtypeStruct((16, width), F32),
        ],
        scratch_shapes=[pltpu.VMEM((2 + nz, 16, width), F32)] + exchange_scratch(1, nz, r, width, 2 + nz),
        compiler_params=params(collective_id=2, has_side_effects=True),
        cost_estimate=cost(6 * rows * width * width, 16 * rows * width),
        name="input_grad_exchange",
    )(x, dq, dk, dv, dr, ab, vecs, *smalls, *halves)


def per_device(
    tokens, lengths, cells, cotangent, ln1_gain, ln1_bias, w_qkv, b_query, b_value, w_out, b_out,
    ln2_gain, ln2_bias, w_up, b_up, w_down, b_down,
):
    seqs, context, width = tokens.shape
    r = w_qkv.shape[0]
    nf = width // r
    nz = nf // 2
    f = lax.axis_index("fsdp")
    ids = jnp.stack([lax.axis_index("dp"), f // 2, f % 2]).astype(jnp.int32)
    vectors = (ln1_gain, ln1_bias, b_query, b_value, b_out, ln2_gain, ln2_bias, b_down, b_up)
    flat = jnp.concatenate(vectors)
    small_rows = -(-flat.shape[0] // 2048) * 16
    small = jnp.pad(flat, (0, small_rows * 128 - flat.shape[0])).reshape(small_rows, 128)
    own = jnp.stack(
        [w_qkv[:, i * width : (i + 1) * width] for i in range(3)]
        + [w_out]
        + [w_up[:, i * width : (i + 1) * width] for i in range(4)]
        + [w_down[i * r : (i + 1) * r] for i in range(4)]
    )
    ab, down_full, smalls = gather_weights(own, small, nz)
    ab = ab.reshape(8, width, width)
    down_full = down_full.reshape(4 * width, width)
    smalls = smalls.reshape(nf, -1).astype(F32)
    vecs = smalls[:, : 8 * r].reshape(nf, 8, r).transpose(1, 0, 2).reshape(8, width)
    bu = smalls[:, 8 * r : 12 * r].reshape(1, 4 * width)
    x = tokens[0]
    kbias, rbias, valid = mask_terms(lengths, cells, context)
    a1, qkv = qkv_forward(x, ab, vecs, 0.125)
    o, qa = attn_forward(qkv, kbias, rbias)
    out, dm, a2, g, du, dr, dy, do, s_g2, s_h2, s_bu, s_bd, s_bo = mlp_both(
        x, o, cotangent[0], valid, ab, down_full, vecs, bu
    )
    down_halves = grad_down_split(ids, g, dm, nz)
    up_halves = grad_up_split(ids, a2, du, nz)
    dq, dk, dv, grad_up, grad_down = attn_backward_exchange(
        qa, qkv, o, do, kbias, up_halves, down_halves, nz
    )
    attn_halves = grad_attn_split(ids, a1, o, dq, dk, dv, dy, nz)
    grad_x, grad_qkv, grad_out, sums = input_grad_exchange(
        x, dq, dk, dv, dr, ab, vecs, (s_bo, s_g2, s_h2, s_bd, s_bu), attn_halves, nz
    )
    mine = lax.dynamic_slice(sums, (0, f * r), (8, r))
    g_g1, g_h1, g_bq, g_bv, g_bo, g_g2, g_h2, g_bd = (mine[i] for i in range(8))
    g_bu = lax.dynamic_slice(sums[8:12].reshape(-1), (f * 4 * r,), (4 * r,))
    return (
        out[None], grad_x[None], g_g1, g_h1, grad_qkv, g_bq, g_bv, grad_out, g_bo, g_g2, g_h2,
        grad_up, g_bu, grad_down, g_bd,
    )


def solution(mesh):
    split = P(("dp", "fsdp"), None, None)
    vec, mat = P("fsdp"), P("fsdp", None)
    in_specs = (
        split, P(("dp", "fsdp")), P(("dp", "fsdp"), None), split,
        vec, vec, mat, vec, vec, mat, vec, vec, vec, mat, vec, mat, vec,
    )
    out_specs = (split, split, vec, vec, mat, vec, vec, mat, vec, vec, vec, mat, vec, mat, vec)
    return jax.shard_map(
        per_device, mesh=mesh, in_specs=in_specs, out_specs=out_specs, check_vma=False
    )
```

```python
from functools import partial
import math

import jax
import jax.numpy as jnp
from jax import lax
from jax.experimental import pallas as pl
from jax.experimental.pallas import tpu as pltpu
from jax.sharding import PartitionSpec as P

HEADS = 12
EPSILON = 1e-05
GELU_C = 0.7978845608028654
GELU_A = 0.044715
MASKED = -1e30
TILE = 256
VMEM_BYTES = 60 * 1024 * 1024
F32 = jnp.float32
BF16 = jnp.bfloat16


def mm(a, b):
    return jnp.dot(a, b, preferred_element_type=F32)


def mm_nt(a, b):
    return lax.dot_general(a, b, (((1,), (1,)), ((), ())), preferred_element_type=F32)


def mm_tn(a, b):
    return lax.dot_general(a, b, (((0,), (0,)), ((), ())), preferred_element_type=F32)


def params(**kw):
    return pltpu.CompilerParams(
        dimension_semantics=("arbitrary",), vmem_limit_bytes=VMEM_BYTES, **kw
    )


def cost(flops, bytes_accessed, transcendentals=0):
    return pl.CostEstimate(
        flops=int(flops), bytes_accessed=int(bytes_accessed), transcendentals=int(transcendentals)
    )


def norm_forward(values):
    row_mean = jnp.mean(values, axis=-1, keepdims=True)
    centered = values - row_mean
    inv_std = lax.rsqrt(jnp.mean(centered * centered, axis=-1, keepdims=True) + EPSILON)
    return centered * inv_std, inv_std


def norm_backward(grad_normed, normalized, inv_std, gain):
    scaled = grad_normed * gain
    return inv_std * (
        scaled
        - jnp.mean(scaled, axis=-1, keepdims=True)
        - normalized * jnp.mean(scaled * normalized, axis=-1, keepdims=True)
    )


def gelu_pair(u):
    square = u * u
    tanh_part = jnp.tanh(u * (GELU_C + (GELU_C * GELU_A) * square))
    half = 0.5 + 0.5 * tanh_part
    value = u * half
    slope = half + value * (1.0 - tanh_part) * (GELU_C + (3.0 * GELU_C * GELU_A) * square)
    return value, slope


def whole(shape):
    return pl.BlockSpec(shape, lambda i: (0,) * len(shape), pipeline_mode=pl.Buffered(1))


def rows_spec(tile, width):
    return pl.BlockSpec((tile, width), lambda i: (i, 0))


def qkv_kernel(scale, x_ref, w_ref, vec_ref, a1_ref, qkv_ref):
    width = x_ref.shape[1]
    gain, shift, bq, bv = (vec_ref[i : i + 1, :] for i in range(4))
    xhat, _ = norm_forward(x_ref[...].astype(F32))
    a1 = (xhat * gain + shift).astype(BF16)
    a1_ref[...] = a1
    q = mm(a1, w_ref[0])
    qkv_ref[:, 0:width] = ((q + bq) * scale).astype(BF16)
    k = mm(a1, w_ref[1])
    qkv_ref[:, width : 2 * width] = k.astype(BF16)
    v = mm(a1, w_ref[2])
    qkv_ref[:, 2 * width : 3 * width] = (v + bv).astype(BF16)


def qkv_forward(x, ab, vecs, scale):
    rows, width = x.shape
    return pl.pallas_call(
        partial(qkv_kernel, scale),
        grid=(rows // TILE,),
        in_specs=[rows_spec(TILE, width), whole((3, width, width)), whole(vecs.shape)],
        out_specs=[rows_spec(TILE, width), rows_spec(TILE, 3 * width)],
        out_shape=[
            jax.ShapeDtypeStruct((rows, width), BF16),
            jax.ShapeDtypeStruct((rows, 3 * width), BF16),
        ],
        compiler_params=params(),
        cost_estimate=cost(6 * rows * width * width, 12 * rows * width),
        name="qkv_forward",
    )(x, ab, vecs)


def split3(value):
    first = value.astype(BF16)
    rest = value - first.astype(F32)
    second = rest.astype(BF16)
    third = (rest - second.astype(F32)).astype(BF16)
    return first, second, third


def attn_fwd_kernel(q_ref, k_ref, v_ref, kbias_ref, rbias_ref, o_ref, qa_ref, mask_ref, between=None):
    blocks = q_ref.shape[0] // TILE
    lane = lax.broadcasted_iota(jnp.int32, (1, 128), 1)

    @pl.when((pl.program_id(0) == 0) & (between is None))
    def _():
        row = lax.broadcasted_iota(jnp.int32, (TILE, TILE), 0)
        col = lax.broadcasted_iota(jnp.int32, (TILE, TILE), 1)
        for i in range(blocks):
            usable = rbias_ref[:, i * TILE : (i + 1) * TILE]
            mask_ref[i] = jnp.where(row == col, 0.0, jnp.where(row > col, usable, MASKED))

    zero = jnp.zeros((), BF16)
    one = jnp.ones((), BF16)
    for head in range(2):
        base = 64 * head
        extra = 64 - base
        own = (lane >= base) & (lane < base + 64)
        if between is not None:
            between(head)
        k_off = jnp.where(own, k_ref[...], jnp.where(lane == extra, kbias_ref[...], zero))
        for i in range(blocks):
            here = slice(i * TILE, (i + 1) * TILE)
            q = jnp.where(own, q_ref[here, :], zero)
            q_off = jnp.where(lane == extra, one, q)
            s_diag = mm_nt(q, k_ref[here, :]) + mask_ref[i]
            row_max = jnp.max(s_diag, axis=-1, keepdims=True)
            if i:
                s_off = mm_nt(q_off, k_off[: i * TILE])
                row_max = jnp.maximum(row_max, jnp.max(s_off, axis=-1, keepdims=True))
            e_diag = jnp.exp(s_diag - row_max)
            total = jnp.sum(e_diag, axis=-1, keepdims=True)
            o = mm(e_diag.astype(BF16), v_ref[here, :])
            if i:
                e_off = jnp.exp(s_off - row_max)
                total += jnp.sum(e_off, axis=-1, keepdims=True)
                o += mm(e_off.astype(BF16), v_ref[0 : i * TILE, :])
            o = (o * (1.0 / total)).astype(BF16)
            if head:
                o_ref[here, :] = jnp.where(own, o, o_ref[here, :])
            else:
                o_ref[here, :] = o
            first, second, third = split3(-(row_max + jnp.log(total)))
            qa = jnp.where(lane == extra + 1, first, q_off)
            qa = jnp.where(lane == extra + 2, second, qa)
            qa = jnp.where(lane == extra + 3, third, qa)
            qa_ref[here, 128 * head : 128 * head + 128] = qa


def attn_forward(qkv, kbias, rbias):
    rows = qkv.shape[0]
    width = qkv.shape[1] // 3
    pairs = width // 128

    def part(p):
        return pl.BlockSpec((rows, 128), lambda i: (0, p * pairs + i))

    return pl.pallas_call(
        attn_fwd_kernel,
        grid=(pairs,),
        in_specs=[part(0), part(1), part(2), whole(kbias.shape), whole(rbias.shape)],
        out_specs=[part(0), pl.BlockSpec((rows, 256), lambda i: (0, i))],
        out_shape=[
            jax.ShapeDtypeStruct((rows, width), BF16),
            jax.ShapeDtypeStruct((rows, 2 * width), BF16),
        ],
        scratch_shapes=[pltpu.VMEM((rows // TILE, TILE, TILE), F32)],
        compiler_params=params(),
        cost_estimate=cost(8 * rows * rows * width, 12 * rows * width),
        name="attn_forward",
    )(qkv, qkv, qkv, kbias, rbias)


def attn_bwd_kernel(
    qa_ref, k_ref, v_ref, o_ref, do_ref, kbias_ref, dq_ref, dk_ref, dv_ref, mask_ref, doa_ref, dqt_ref,
    between=None,
):
    rows = k_ref.shape[0]
    blocks = rows // TILE
    lane = lax.broadcasted_iota(jnp.int32, (1, 128), 1)

    @pl.when(pl.program_id(0) == 0)
    def _():
        key = lax.broadcasted_iota(jnp.int32, (TILE, TILE), 0)
        query = lax.broadcasted_iota(jnp.int32, (TILE, TILE), 1)
        for i in range(blocks):
            usable = kbias_ref[i * TILE : (i + 1) * TILE, 0:1].astype(F32)
            mask_ref[i] = jnp.where(key == query, 0.0, jnp.where(query > key, usable, MASKED))

    zero = jnp.zeros((), BF16)
    one = jnp.ones((), BF16)
    product = do_ref[...].astype(F32) * o_ref[...].astype(F32)
    kt = k_ref[...].T
    for head in range(2):
        base = 64 * head
        extra = 64 - base
        own = (lane >= base) & (lane < base + 64)
        terms = (lane > extra) & (lane <= extra + 3)
        qa_cols = slice(128 * head, 128 * head + 128)
        if between is not None:
            between(head)
        inner = -jnp.sum(jnp.where(own, product, 0.0), axis=-1, keepdims=True)
        first, second, third = split3(inner)
        doa = jnp.where(own, do_ref[...], zero)
        doa = jnp.where(lane == extra + 1, first, doa)
        doa = jnp.where(lane == extra + 2, second, doa)
        doa_ref[...] = jnp.where(lane == extra + 3, third, doa)
        for j in range(blocks):
            here = slice(j * TILE, (j + 1) * TILE)
            after = slice((j + 1) * TILE, rows)
            k_diag = jnp.where(own, k_ref[here, :], jnp.where(terms, one, zero))
            v_aug = jnp.where(own, v_ref[here, :], jnp.where(terms, one, zero))
            p_diag = jnp.exp(mm_nt(k_diag, qa_ref[here, qa_cols]) + mask_ref[j])
            dp_diag = mm_nt(v_aug, doa_ref[here, :])
            ds_diag = (p_diag * dp_diag).astype(BF16)
            dv = mm(p_diag.astype(BF16), do_ref[here, :])
            dk = mm(ds_diag, qa_ref[here, qa_cols])
            dq_diag = mm(kt[:, here], ds_diag)
            if j:
                dqt_ref[:, here] += dq_diag
            else:
                dqt_ref[:, here] = dq_diag
            if j + 1 < blocks:
                k_off = jnp.where(lane == extra, kbias_ref[here, :], k_diag)
                p_off = jnp.exp(mm_nt(k_off, qa_ref[after, qa_cols]))
                dp_off = mm_nt(v_aug, doa_ref[after, :])
                ds_off = (p_off * dp_off).astype(BF16)
                dv += mm(p_off.astype(BF16), do_ref[after, :])
                dk += mm(ds_off, qa_ref[after, qa_cols])
                dq_off = mm(kt[:, here], ds_off)
                if j:
                    dqt_ref[:, after] += dq_off
                else:
                    dqt_ref[:, after] = dq_off
            dk = dk.astype(BF16)
            dv = dv.astype(BF16)
            if head:
                dk_ref[here, :] = jnp.where(own, dk, dk_ref[here, :])
                dv_ref[here, :] = jnp.where(own, dv, dv_ref[here, :])
            else:
                dk_ref[here, :] = dk
                dv_ref[here, :] = dv
        dq = (dqt_ref[...] * 0.125).astype(BF16).T
        if head:
            dq_ref[...] = jnp.where(own, dq, dq_ref[...])
        else:
            dq_ref[...] = dq


def mlp_kernel(
    x_ref, o_ref, cot_ref, length_ref, wo_ref, wu_ref, wd_ref, vec_ref, bu_ref,
    out_ref, dm_ref, a2_ref, g_ref, du_ref, dr_ref, dy_ref, do_ref,
    s_gain_ref, s_shift_ref, s_bu_ref, s_bd_ref, s_bo_ref,
):
    chunk = wu_ref.shape[2]
    hidden = wd_ref.shape[0]
    bo, gain, shift, bd = (vec_ref[i : i + 1, :] for i in range(4, 8))
    middle = x_ref[...].astype(F32) + mm(o_ref[...], wo_ref[0]) + bo
    xhat, inv_std = norm_forward(middle)
    a2 = (xhat * gain + shift).astype(BF16)
    a2_ref[...] = a2
    row = lax.broadcasted_iota(jnp.int32, middle.shape, 0) + pl.program_id(0) * middle.shape[0]
    dout = jnp.where(row < length_ref[0], cot_ref[...].astype(F32), 0.0)
    dm = dout.astype(BF16)
    dm_ref[...] = dm
    out = middle + bd
    da2 = jnp.zeros_like(middle)
    first = pl.program_id(0) == 0

    def add_sum(ref, cols, value):
        part = jnp.sum(value, axis=0, keepdims=True)
        ref[:, cols] = jnp.where(first, part, ref[:, cols] + part)

    for c in range(hidden // chunk):
        cols = slice(c * chunk, (c + 1) * chunk)
        u = mm(a2, wu_ref[c]) + bu_ref[:, cols]
        value, slope = gelu_pair(u)
        g = value.astype(BF16)
        g_ref[:, cols] = g
        out += mm(g, wd_ref[cols, :])
        du = (mm_nt(dm, wd_ref[cols, :]) * slope).astype(BF16)
        du_ref[:, cols] = du
        add_sum(s_bu_ref, cols, du.astype(F32))
        da2 += mm_nt(du, wu_ref[c])
    out_ref[...] = out.astype(BF16)
    every = slice(None)
    add_sum(s_bd_ref, every, dm.astype(F32))
    add_sum(s_gain_ref, every, da2 * xhat)
    add_sum(s_shift_ref, every, da2)
    dr = dout + norm_backward(da2, xhat, inv_std, gain)
    dr_ref[...] = dr
    dy = dr.astype(BF16)
    dy_ref[...] = dy
    add_sum(s_bo_ref, every, dy.astype(F32))
    do_ref[...] = mm_nt(dy, wo_ref[0]).astype(BF16)


def mlp_both(x, o, cot, lengths, ab, w_down, vecs, b_up):
    rows, width = x.shape
    hidden = w_down.shape[0]
    row = rows_spec(TILE, width)
    wide = rows_spec(TILE, hidden)
    acc = pl.BlockSpec((1, width), lambda i: (0, 0))
    acc_wide = pl.BlockSpec((1, hidden), lambda i: (0, 0))

    def shape(r, c, t):
        return jax.ShapeDtypeStruct((r, c), t)

    return pl.pallas_call(
        mlp_kernel,
        grid=(rows // TILE,),
        in_specs=[
            row, row, row, pl.BlockSpec(memory_space=pltpu.SMEM),
            pl.BlockSpec((1, width, width), lambda i: (3, 0, 0), pipeline_mode=pl.Buffered(1)),
            pl.BlockSpec((4, width, width), lambda i: (1, 0, 0), pipeline_mode=pl.Buffered(1)),
            whole(w_down.shape), whole(vecs.shape), whole(b_up.shape),
        ],
        out_specs=[row, row, row, wide, wide, row, row, row, acc, acc, acc_wide, acc, acc],
        out_shape=[
            shape(rows, width, BF16), shape(rows, width, BF16), shape(rows, width, BF16),
            shape(rows, hidden, BF16), shape(rows, hidden, BF16), shape(rows, width, F32),
            shape(rows, width, BF16), shape(rows, width, BF16),
            shape(1, width, F32), shape(1, width, F32), shape(1, hidden, F32),
            shape(1, width, F32), shape(1, width, F32),
        ],
        compiler_params=params(),
        cost_estimate=cost(rows * width * (8 * hidden + 4 * width), 24 * rows * width + 12 * rows * hidden),
        name="mlp_both",
    )(x, o, cot, lengths, ab, ab, w_down, vecs, b_up)


def mask_terms(lengths, cells, context):
    usable = (jnp.arange(context) < lengths[0]) & (cells[0] == 1)
    bias = jnp.where(usable, 0.0, MASKED)
    return jnp.broadcast_to(bias.astype(BF16)[:, None], (context, 128)), bias[None, :]


def gather_kernel(nz, n_small, own_ref, small_ref, ab_ref, c_ref, all_small_ref, send, recv, local):
    d = lax.axis_index("dp")
    f = lax.axis_index("fsdp")
    z, c = f // 2, f % 2
    half = own_ref.shape[2] // 2
    mate = z * 2 + (1 - c)
    flip_x = d + 1 - 2 * (d % 2)
    flip_y = lax.rem(d + 2, 4)
    flip_xy = lax.rem(flip_x + 2, 4)
    others = [lax.rem(z + k, nz) for k in range(1, nz)]

    barrier = pltpu.get_barrier_semaphore()
    partners = [(flip_x, f), (flip_y, f), (d, mate)]
    for o in others:
        partners += [(d, o * 2 + c), (d, o * 2 + 1 - c)]
    for p in partners:
        pl.semaphore_signal(barrier, inc=1, device_id=p, device_id_type=pl.DeviceIdType.MESH)
    pl.semaphore_wait(barrier, len(partners))

    def slot(g, block, shard):
        if g == 2:
            return c_ref.at[shard, block]
        return ab_ref.at[g * 4 + block, shard]

    count = [0]
    pending = []

    def copy(src, dst, device, last=True):
        s = count[0]
        count[0] += 1
        made = pltpu.make_async_remote_copy(
            src_ref=src, dst_ref=dst, send_sem=send.at[s], recv_sem=recv.at[s],
            device_id=device, device_id_type=pl.DeviceIdType.MESH,
        )
        made.start()
        if last:
            pending.append(made)
        return made

    def left(ref):
        return ref.at[:, 0:half]

    def right(ref):
        return ref.at[:, half : 2 * half]

    fetch = {}
    for o in others:
        copy(small_ref, all_small_ref.at[f], (d, o * 2 + c))
        copy(small_ref, all_small_ref.at[f], (d, o * 2 + 1 - c))
    copy(small_ref, all_small_ref.at[f], (d, mate))
    for g in range(3):
        for k, o in enumerate(others):
            fetch[g, k] = copy(own_ref.at[g * 4 + d], slot(g, d, f), (d, o * 2 + c), False)
    copy(own_ref.at[0:8], ab_ref.at[:, f], (d, mate))
    copy(own_ref.at[8:12], c_ref.at[f], (d, mate))
    keep = [
        pltpu.make_async_copy(own_ref.at[0:8], ab_ref.at[:, f], local.at[0]),
        pltpu.make_async_copy(own_ref.at[8:12], c_ref.at[f], local.at[1]),
        pltpu.make_async_copy(small_ref, all_small_ref.at[f], local.at[2]),
    ]
    for made in keep:
        made.start()
    arrived = list(fetch.values())

    units = [(g, k) for g in range(3) for k in range(nz - 1)]
    by_x, by_y, corner = {}, {}, {}
    for step in range(len(units) + 2):
        if step < len(units):
            g, k = units[step]
            shard = lax.rem(z + nz - 1 - k, nz) * 2 + c
            fetch[g, k].wait_recv()
            mine = slot(g, d, shard)
            by_x[step] = copy(mine, mine, (flip_x, f), False)
            by_y[step] = copy(mine, mine, (flip_y, f), False)
            copy(mine, mine, (d, mate))
        if 1 <= step <= len(units):
            g, k = units[step - 1]
            shard = lax.rem(z + nz - 1 - k, nz) * 2 + c
            by_x[step - 1].wait_recv()
            theirs = slot(g, flip_x, shard)
            first = copy(right(theirs), right(theirs), (flip_y, f), False)
            copy(theirs, theirs, (d, mate))
            by_y[step - 1].wait_recv()
            theirs = slot(g, flip_y, shard)
            second = copy(left(theirs), left(theirs), (flip_x, f), False)
            copy(theirs, theirs, (d, mate))
            corner[step - 1] = (first, second)
        if step >= 2:
            g, k = units[step - 2]
            shard = lax.rem(z + nz - 1 - k, nz) * 2 + c
            for made in corner[step - 2]:
                made.wait_recv()
            theirs = slot(g, flip_xy, shard)
            copy(theirs, theirs, (d, mate))
    arrived += list(by_x.values()) + list(by_y.values())
    arrived += [made for both in corner.values() for made in both]
    for made in arrived:
        made.wait_send()
    for made in pending:
        made.wait()
    for made in keep:
        made.wait()


def gather_copies(nz):
    return (2 * (nz - 1) + 1) + 3 * (nz - 1) + 2 + 3 * (nz - 1) * 8


def gather_weights(own, small, nz):
    r, width = own.shape[1:]
    copies = gather_copies(nz)
    any_spec = pl.BlockSpec(memory_space=pl.ANY)
    vmem = pl.BlockSpec(memory_space=pltpu.VMEM)
    return pl.pallas_call(
        partial(gather_kernel, nz, small.shape[0]),
        in_specs=[vmem, vmem],
        out_specs=[any_spec, any_spec, any_spec],
        out_shape=[
            jax.ShapeDtypeStruct((8, 2 * nz, r, width), BF16),
            jax.ShapeDtypeStruct((2 * nz, 4, r, width), BF16),
            jax.ShapeDtypeStruct((2 * nz,) + small.shape, BF16),
        ],
        scratch_shapes=[
            pltpu.SemaphoreType.DMA((copies,)),
            pltpu.SemaphoreType.DMA((copies,)),
            pltpu.SemaphoreType.DMA((3,)),
        ],
        compiler_params=pltpu.CompilerParams(
            collective_id=0, has_side_effects=True, vmem_limit_bytes=16 * 1024 * 1024
        ),
        name="gather_weights",
    )(own, small)


def head_kernel(
    nz, slots_of, wqkv_ref, wout_ref, wup_ref, wdown_ref, small_ref, x_ref, cells_ref, length_ref,
    ab_ref, c_ref, vecs_ref, bu_ref, kbias_ref, a1_ref, qkv_ref, o_ref, qa_ref,
    own, attn_w, up_w, down_w, rbias_ref, all_small, mask_ref, send, recv, local,
):
    pid = pl.program_id(0)
    d = lax.axis_index("dp")
    f = lax.axis_index("fsdp")
    z, c = f // 2, f % 2
    r, width = own.shape[1:]
    half = width // 2
    rows = x_ref.shape[0]
    mate = z * 2 + (1 - c)
    flip_x = d + 1 - 2 * (d % 2)
    flip_y = lax.rem(d + 2, 4)
    flip_xy = lax.rem(flip_x + 2, 4)
    others = [lax.rem(z + k, nz) for k in range(1, nz)]

    def slot(g, block, shard):
        if g == 0:
            return attn_w.at[block, shard]
        if g == 1:
            return up_w.at[block, shard]
        return down_w.at[shard, block]

    def remote(src, dst, index, device):
        return pltpu.make_async_remote_copy(
            src_ref=src, dst_ref=dst, send_sem=send.at[index], recv_sem=recv.at[index],
            device_id=device, device_id_type=pl.DeviceIdType.MESH,
        )

    units = [(g, k) for g in range(3) for k in range(nz - 1)]
    own_base = len(units) * 9
    small_base = own_base + 3

    def shard_of(k):
        return lax.rem(z + nz - 1 - k, nz) * 2 + c

    def fetch(u):
        g, k = units[u]
        return remote(own.at[g * 4 + d], slot(g, d, f), u * 9, (d, others[k] * 2 + c))

    def stage_one(u):
        g, k = units[u]
        mine = slot(g, d, shard_of(k))
        return [
            remote(mine, mine, u * 9 + 1, (flip_x, f)),
            remote(mine, mine, u * 9 + 2, (flip_y, f)),
            remote(mine, mine, u * 9 + 3, (d, mate)),
        ]

    def stage_two(u):
        g, k = units[u]
        from_x, from_y = slot(g, flip_x, shard_of(k)), slot(g, flip_y, shard_of(k))
        right, left = from_x.at[:, half : 2 * half], from_y.at[:, 0:half]
        return [
            remote(right, right, u * 9 + 4, (flip_y, f)),
            remote(from_x, from_x, u * 9 + 5, (d, mate)),
            remote(left, left, u * 9 + 6, (flip_x, f)),
            remote(from_y, from_y, u * 9 + 7, (d, mate)),
        ]

    def stage_three(u):
        g, k = units[u]
        corner = slot(g, flip_xy, shard_of(k))
        return remote(corner, corner, u * 9 + 8, (d, mate))

    def own_copies():
        return [
            remote(own.at[0:4], attn_w.at[:, f], own_base, (d, mate)),
            remote(own.at[4:8], up_w.at[:, f], own_base + 1, (d, mate)),
            remote(own.at[8:12], down_w.at[f], own_base + 2, (d, mate)),
        ]

    def own_keeps():
        return [
            pltpu.make_async_copy(own.at[0:4], attn_w.at[:, f], local.at[0]),
            pltpu.make_async_copy(own.at[4:8], up_w.at[:, f], local.at[1]),
            pltpu.make_async_copy(own.at[8:12], down_w.at[f], local.at[2]),
        ]

    def small_copies():
        there = [(d, o * 2 + e) for o in others for e in (c, 1 - c)] + [(d, mate)]
        return [remote(small_ref, all_small.at[f], small_base + i, p) for i, p in enumerate(there)]

    def outward(g):
        if g == 0:
            return pltpu.make_async_copy(attn_w, ab_ref.at[0:4], local.at[3])
        if g == 1:
            return pltpu.make_async_copy(up_w, ab_ref.at[4:8], local.at[4])
        return pltpu.make_async_copy(down_w, c_ref, local.at[17])

    def event(t, lo, hi):
        if lo <= t < hi:
            fetch(t).wait_recv()
            if t < nz - 1:
                fetch(nz - 1 + t).start()
            for made in stage_one(t):
                made.start()
        if lo <= t - 1 < hi:
            one, two = stage_one(t - 1), stage_two(t - 1)
            one[0].wait_recv()
            two[0].start()
            two[1].start()
            one[1].wait_recv()
            two[2].start()
            two[3].start()
        if lo <= t - 2 < hi:
            two = stage_two(t - 2)
            two[0].wait_recv()
            two[2].wait_recv()
            stage_three(t - 2).start()

    def mates_done(lo, hi):
        for u in range(lo, hi):
            stage_one(u)[2].wait_recv()
            stage_two(u)[1].wait_recv()
            stage_two(u)[3].wait_recv()
            stage_three(u).wait_recv()

    @pl.when(pid == 0)
    def _():
        fill = []
        for i in range(12):
            if i < 3:
                src = wqkv_ref.at[:, i * width : (i + 1) * width]
            elif i == 3:
                src = wout_ref
            elif i < 8:
                src = wup_ref.at[:, (i - 4) * width : (i - 3) * width]
            else:
                src = wdown_ref.at[(i - 8) * r : (i - 7) * r, :]
            fill.append(pltpu.make_async_copy(src, own.at[i], local.at[5 + i]))
        for made in fill:
            made.start()
        barrier = pltpu.get_barrier_semaphore()
        partners = [(flip_x, f), (flip_y, f), (d, mate)]
        for o in others:
            partners += [(d, o * 2 + c), (d, o * 2 + 1 - c)]
        for p in partners:
            pl.semaphore_signal(barrier, inc=1, device_id=p, device_id_type=pl.DeviceIdType.MESH)
        for made in fill:
            made.wait()
        pl.semaphore_wait(barrier, len(partners))
        for made in small_copies():
            made.start()
        for u in range(nz - 1):
            fetch(u).start()
        for made in own_copies() + own_keeps():
            made.start()
        all_small[f] = small_ref[...]

        usable = (lax.broadcasted_iota(jnp.int32, (1, rows), 1) < length_ref[0]) & (cells_ref[...] == 1)
        rbias_ref[...] = jnp.where(usable, 0.0, MASKED)
        kbias_ref[...] = jnp.broadcast_to(rbias_ref[...], (128, rows)).T.astype(BF16)
        row = lax.broadcasted_iota(jnp.int32, (TILE, TILE), 0)
        col = lax.broadcasted_iota(jnp.int32, (TILE, TILE), 1)
        for i in range(rows // TILE):
            keys = rbias_ref[:, i * TILE : (i + 1) * TILE]
            mask_ref[i] = jnp.where(row == col, 0.0, jnp.where(row > col, keys, MASKED))

        for made in small_copies():
            made.wait_recv()
        lane = lax.broadcasted_iota(jnp.int32, (128, width), 0)
        at = lax.broadcasted_iota(jnp.int32, (128, width), 1)
        vecs = jnp.zeros((16, width), F32)
        for shard in range(2 * nz):
            spot = ((at == lane + shard * r) & (lane < r)).astype(BF16)
            vecs += mm(all_small[shard], spot)
        vecs_ref[...] = vecs
        lane = lax.broadcasted_iota(jnp.int32, (128, 4 * r), 0)
        at = lax.broadcasted_iota(jnp.int32, (128, 4 * r), 1)
        for shard in range(2 * nz):
            part = jnp.zeros((16, 4 * r), F32)
            for j in range(4):
                spot = ((at == lane + j * r) & (lane < r)).astype(BF16)
                part = part + mm(pltpu.roll(all_small[shard].astype(F32), 8 - j, 0).astype(BF16), spot)
            bu_ref[:, shard * 4 * r : (shard + 1) * 4 * r] = part[0:1]
        gain, shift = vecs_ref[0:1, :], vecs_ref[1:2, :]
        for i in range(rows // TILE):
            here = slice(i * TILE, (i + 1) * TILE)
            xhat, _ = norm_forward(x_ref[here, :].astype(F32))
            a1_ref[here, :] = (xhat * gain + shift).astype(BF16)

        for t in range(nz + 1):
            event(t, 0, nz - 1)
        own_copies()[0].wait_recv()
        own_keeps()[0].wait()
        mates_done(0, nz - 1)
        outward(0).start()
        for u in range(2 * nz - 2, len(units)):
            fetch(u).start()

    def between(index):
        if index == 15:
            mates_done(nz - 1, 2 * nz - 2)
            own_copies()[1].wait_recv()
            own_keeps()[1].wait()
            outward(1).start()
        for t in slots_of.get(index, ()):
            event(nz - 1 + t, nz - 1, len(units))

    for i in range(4):
        @pl.when(pid == 1 + i)
        def _():
            between(i)

    @pl.when((pid >= 1) & (pid < 5))
    def _():
        size = rows // 4
        here = pl.ds(pl.multiple_of((pid - 1) * size, size), size)
        a1 = a1_ref[here, :]
        bq, bv = vecs_ref[2:3, :], vecs_ref[3:4, :]
        q = mm(a1, attn_w[0].reshape(width, width))
        qkv_ref[here, 0:width] = ((q + bq) * 0.125).astype(BF16)
        k = mm(a1, attn_w[1].reshape(width, width))
        qkv_ref[here, width : 2 * width] = k.astype(BF16)
        v = mm(a1, attn_w[2].reshape(width, width))
        qkv_ref[here, 2 * width : 3 * width] = (v + bv).astype(BF16)

    def between_heads(head):
        for pair in range(6):
            if 4 + 2 * pair + head in slots_of or 4 + 2 * pair + head == 15:
                @pl.when(pid == 5 + pair)
                def _():
                    between(4 + 2 * pair + head)

    @pl.when(pid >= 5)
    def _():
        cols = [pl.ds(pl.multiple_of(p * width + (pid - 5) * 128, 128), 128) for p in range(3)]
        attn_fwd_kernel(
            qkv_ref.at[:, cols[0]], qkv_ref.at[:, cols[1]], qkv_ref.at[:, cols[2]], kbias_ref, rbias_ref,
            o_ref, qa_ref, mask_ref, between=between_heads,
        )

    @pl.when(pid == 10)
    def _():
        between(16)
        mates_done(2 * nz - 2, len(units))
        own_copies()[2].wait_recv()
        own_keeps()[2].wait()
        outward(2).start()
        for g in range(3):
            outward(g).wait()
        for u in range(len(units)):
            fetch(u).wait_send()
            for made in stage_one(u) + stage_two(u) + [stage_three(u)]:
                made.wait_send()
        for made in own_copies() + small_copies():
            made.wait_send()


SLOTS = {1: (0,), 3: (1,), 5: (2,), 7: (3,), 9: (4,), 11: (5,), 13: (6,), 15: (7,)}


def head_forward(w_qkv, w_out, w_up, w_down, small, x, cells, lengths, nz):
    rows, width = x.shape
    r = w_qkv.shape[0]
    copies = 3 * (nz - 1) * 9 + 3 + 2 * nz - 1
    any_spec = pl.BlockSpec(memory_space=pl.ANY)
    events = 2 * (nz - 1) + 2
    slots_of = SLOTS if nz == 4 else {}
    if not slots_of:
        for t in range(events):
            slots_of.setdefault(t * 16 // events, []).append(t)

    def shape(*s, t=BF16):
        return jax.ShapeDtypeStruct(s, t)

    return pl.pallas_call(
        partial(head_kernel, nz, slots_of),
        grid=(11,),
        in_specs=[any_spec] * 4 + [
            whole(small.shape), whole(x.shape), whole(cells.shape), pl.BlockSpec(memory_space=pltpu.SMEM),
        ],
        out_specs=[
            any_spec, any_spec, whole((16, width)), whole((1, 4 * width)), whole((rows, 128)),
            whole((rows, width)), whole((rows, 3 * width)),
            pl.BlockSpec((rows, 128), lambda i: (0, jnp.maximum(i - 5, 0))),
            pl.BlockSpec((rows, 256), lambda i: (0, jnp.maximum(i - 5, 0))),
        ],
        out_shape=[
            shape(8, 2 * nz, r, width), shape(2 * nz, 4, r, width), shape(16, width, t=F32),
            shape(1, 4 * width, t=F32), shape(rows, 128), shape(rows, width), shape(rows, 3 * width),
            shape(rows, width), shape(rows, 2 * width),
        ],
        scratch_shapes=[
            pltpu.VMEM((12, r, width), BF16),
            pltpu.VMEM((4, 2 * nz, r, width), BF16),
            pltpu.VMEM((4, 2 * nz, r, width), BF16),
            pltpu.VMEM((2 * nz, 4, r, width), BF16),
            pltpu.VMEM((1, rows), F32),
            pltpu.VMEM((2 * nz, 16, 128), BF16),
            pltpu.VMEM((rows // TILE, TILE, TILE), F32),
            pltpu.SemaphoreType.DMA((copies,)),
            pltpu.SemaphoreType.DMA((copies,)),
            pltpu.SemaphoreType.DMA((18,)),
        ],
        compiler_params=params(collective_id=0, has_side_effects=True),
        cost_estimate=cost(6 * rows * width * width + 8 * rows * rows * width, 24 * rows * width),
        name="head_forward",
    )(w_qkv, w_out, w_up, w_down, small, x, cells, lengths)


def core_split(res_ref, core, r, nz, send_ref, keep_ref):
    for i in range(nz):
        base = i * 2 * r
        send_ref[0, i] = res_ref[pl.ds(pl.multiple_of(base + (1 - core) * r, 8), r), :].astype(BF16)
        keep_ref[0, i] = res_ref[pl.ds(pl.multiple_of(base + core * r, 8), r), :].astype(BF16)


def grad_up_kernel(nz, r, ids_ref, a_ref, b_ref, send_ref, keep_ref, res_ref, at_ref):
    @pl.when(pl.program_id(0) == 0)
    def _():
        at_ref[...] = a_ref[...].T

    res_ref[...] = mm(at_ref[...], b_ref[...])
    core_split(res_ref, ids_ref[2], r, nz, send_ref, keep_ref)


def grad_up_split(ids, a, b, nz):
    rows, m = a.shape
    blocks = b.shape[1] // m
    r = m // (2 * nz)
    half = jax.ShapeDtypeStruct((blocks, nz, r, m), BF16)
    out = pl.BlockSpec((1, nz, r, m), lambda i, ids: (i, 0, 0, 0))
    return pl.pallas_call(
        partial(grad_up_kernel, nz, r),
        grid_spec=pltpu.PrefetchScalarGridSpec(
            num_scalar_prefetch=1,
            grid=(blocks,),
            in_specs=[
                pl.BlockSpec((rows, m), lambda i, ids: (0, 0), pipeline_mode=pl.Buffered(1)),
                pl.BlockSpec((rows, m), lambda i, ids: (0, i)),
            ],
            out_specs=[out, out],
            scratch_shapes=[pltpu.VMEM((m, m), F32), pltpu.VMEM((m, rows), BF16)],
        ),
        out_shape=[half, half],
        compiler_params=params(),
        cost_estimate=cost(2 * rows * m * b.shape[1], 2 * (rows * m + rows * b.shape[1] + m * b.shape[1])),
        name="grad_up",
    )(ids, a, b)


def grad_down_kernel(r, ids_ref, a_ref, b_ref, send_ref, keep_ref, res_ref):
    res_ref[...] = mm_tn(a_ref[...], b_ref[...])
    core = ids_ref[2]
    for j in range(send_ref.shape[1]):
        for i in range(4):
            base = j * 8 * r + i * r
            there = pl.multiple_of(base + (1 - core) * 4 * r, 8)
            here = pl.multiple_of(base + core * 4 * r, 8)
            send_ref[i, j] = res_ref[pl.ds(there, r), :].astype(BF16)
            keep_ref[i, j] = res_ref[pl.ds(here, r), :].astype(BF16)


def grad_down_split(ids, a, b, nz):
    rows, hidden = a.shape
    n = b.shape[1]
    r = hidden // (8 * nz)
    per = hidden // 4
    half = jax.ShapeDtypeStruct((4, nz, r, n), BF16)
    out = pl.BlockSpec((4, nz // 4, r, n), lambda i, ids: (0, i, 0, 0))
    return pl.pallas_call(
        partial(grad_down_kernel, r),
        grid_spec=pltpu.PrefetchScalarGridSpec(
            num_scalar_prefetch=1,
            grid=(4,),
            in_specs=[
                pl.BlockSpec((rows, per), lambda i, ids: (0, i)),
                pl.BlockSpec((rows, n), lambda i, ids: (0, 0), pipeline_mode=pl.Buffered(1)),
            ],
            out_specs=[out, out],
            scratch_shapes=[pltpu.VMEM((per, n), F32)],
        ),
        out_shape=[half, half],
        compiler_params=params(),
        cost_estimate=cost(2 * rows * hidden * n, 2 * (rows * hidden + rows * n + hidden * n)),
        name="grad_down",
    )(ids, a, b)


class Exchange:
    def __init__(self, sends, keeps, late, mine, core_in, x_in, y_in, x2_in, y2_in, z_in, owned, dp_in, sems):
        self.sends, self.keeps = sends, keeps
        self.mine, self.core_in = mine, core_in
        self.x_in, self.y_in, self.x2_in, self.y2_in = x_in, y_in, x2_in, y2_in
        self.z_in, self.owned, self.dp_in = z_in, owned, dp_in
        self.send_sem, self.recv_sem, self.load_sem = sems
        self.groups = len(sends) + 1
        self.late = late
        self.early = len(sends)
        self.nz = mine.shape[0] // self.groups
        self.half = mine.shape[3] // 2
        self.units = self.groups * self.nz
        d = lax.axis_index("dp")
        f = lax.axis_index("fsdp")
        self.d, self.f, self.z, self.c = d, f, f // 2, f % 2
        self.x = d + 1 - 2 * (d % 2)
        self.y = lax.rem(d + 2, 4)
        self.xy = lax.rem(self.x + 2, 4)
        self.mate = self.z * 2 + 1 - self.c

    def barrier(self):
        barrier = pltpu.get_barrier_semaphore()
        partners = [(self.d, self.mate)] + [(p, self.f) for p in (self.x, self.y, self.xy)]
        partners += [(self.d, lax.rem(self.z + k, self.nz) * 2 + self.c) for k in range(1, self.nz)]
        for p in partners:
            pl.semaphore_signal(barrier, inc=1, device_id=p, device_id_type=pl.DeviceIdType.MESH)
        pl.semaphore_wait(barrier, len(partners))

    def remote(self, src, dst, index, device):
        return pltpu.make_async_remote_copy(
            src_ref=src, dst_ref=dst, send_sem=self.send_sem.at[index], recv_sem=self.recv_sem.at[index],
            device_id=device, device_id_type=pl.DeviceIdType.MESH,
        )

    def owner(self, u):
        return lax.rem(self.z + 1 + u % self.nz, self.nz)

    def late_copy(self, block):
        first = self.units - self.nz
        return self.remote(
            self.late.at[block], self.core_in.at[pl.ds(first, self.nz), block], (first + block) * 8,
            (self.d, self.mate),
        )

    def core_copy(self, u):
        src = self.sends[u // self.nz].at[:, self.owner(u)]
        return self.remote(src, self.core_in.at[u], u * 8, (self.d, self.mate))

    def load(self, u):
        src = self.keeps[u // self.nz].at[:, self.owner(u)]
        return pltpu.make_async_copy(src, self.mine.at[u], self.load_sem.at[u])

    def plane_copies(self, u):
        lo, hi = slice(0, self.half), slice(self.half, 2 * self.half)
        m = self.mine.at[u]
        to_x, to_y = (self.x, self.f), (self.y, self.f)
        return [
            self.remote(m.at[self.x, :, lo], self.x_in.at[u, 0], u * 8 + 1, to_x),
            self.remote(m.at[self.y, :, hi], self.y_in.at[u, 0], u * 8 + 2, to_y),
            self.remote(m.at[self.xy, :, lo], self.x_in.at[u, 1], u * 8 + 3, to_x),
            self.remote(m.at[self.xy, :, hi], self.y_in.at[u, 1], u * 8 + 4, to_y),
        ]

    def second_copies(self, u):
        lo, hi = slice(0, self.half), slice(self.half, 2 * self.half)
        m = self.mine.at[u]
        return [
            self.remote(m.at[self.y, :, lo], self.y2_in.at[u], u * 8 + 5, (self.y, self.f)),
            self.remote(m.at[self.x, :, hi], self.x2_in.at[u], u * 8 + 6, (self.x, self.f)),
        ]

    def owner_copy(self, u):
        g, j = u // self.nz, u % self.nz
        return self.remote(
            self.mine.at[u, self.d], self.z_in.at[g, j], u * 8 + 7, (self.d, self.owner(u) * 2 + self.c)
        )

    def dp_copies(self, g):
        base = self.units * 8 + 3 * g
        return [
            self.remote(self.owned.at[g], self.dp_in.at[g, i], base + i, (p, self.f))
            for i, p in enumerate((self.x, self.y, self.xy))
        ]

    def start(self):
        for u in range(AHEAD):
            self.core_copy(u).start()
        for u in range(self.units - self.nz):
            self.load(u).start()

    def add(self, u, block, cols, term):
        value = self.mine[u, block, :, cols].astype(F32) + term.astype(F32)
        self.mine[u, block, :, cols] = value.astype(BF16)

    def stage_one(self, u):
        if u < self.units - self.nz:
            self.load(u).wait()
            self.core_copy(u).wait_recv()
            if u + AHEAD < self.units - self.nz:
                self.core_copy(u + AHEAD).start()
        elif u == self.units - self.nz:
            for block in range(4):
                self.late_copy(block).wait_recv()
        for block in range(4):
            self.add(u, block, slice(None), self.core_in[u, block])
        for made in self.plane_copies(u):
            made.start()

    def stage_two(self, u):
        lo, hi = slice(0, self.half), slice(self.half, 2 * self.half)
        copies = self.plane_copies(u)
        copies[0].wait_recv()
        self.add(u, self.d, lo, self.x_in[u, 0])
        copies[1].wait_recv()
        self.add(u, self.d, hi, self.y_in[u, 0])
        copies[2].wait_recv()
        self.add(u, self.y, lo, self.x_in[u, 1])
        copies[3].wait_recv()
        self.add(u, self.x, hi, self.y_in[u, 1])
        for made in self.second_copies(u):
            made.start()

    def stage_three(self, u):
        lo, hi = slice(0, self.half), slice(self.half, 2 * self.half)
        copies = self.second_copies(u)
        copies[0].wait_recv()
        self.add(u, self.d, lo, self.y2_in[u])
        copies[1].wait_recv()
        self.add(u, self.d, hi, self.x2_in[u])
        if u % self.nz != self.nz - 1:
            self.owner_copy(u).start()

    def stage_four(self, g):
        last = g * self.nz + self.nz - 1
        total = self.mine[last, self.d].astype(F32)
        for j in range(self.nz - 1):
            self.owner_copy(g * self.nz + j).wait_recv()
            total = total + self.z_in[g, j].astype(F32)
        self.owned[g] = total.astype(BF16)
        for made in self.dp_copies(g):
            made.start()

    def blocks(self, g):
        yield self.d, self.owned[g].astype(F32)
        for i, (made, p) in enumerate(zip(self.dp_copies(g), (self.x, self.y, self.xy))):
            made.wait_recv()
            yield p, self.dp_in[g, i].astype(F32)

    def finish(self):
        for u in range(self.units):
            if u < self.units - self.nz:
                self.core_copy(u).wait_send()
            for made in self.plane_copies(u) + self.second_copies(u):
                made.wait_send()
            if u % self.nz != self.nz - 1:
                self.owner_copy(u).wait_send()
        for block in range(4):
            self.late_copy(block).wait_send()
        for g in range(self.groups):
            for made in self.dp_copies(g):
                made.wait_send()

    def steps(self):
        return self.units + LAG_THREE

    def step(self, t):
        if t < self.units:
            self.stage_one(t)
        if LAG_TWO <= t < self.units + LAG_TWO:
            self.stage_two(t - LAG_TWO)
        if LAG_THREE <= t:
            self.stage_three(t - LAG_THREE)
        for g in range(self.groups - 1):
            if t == (g + 1) * self.nz - 1 + LAG_FOUR:
                self.stage_four(g)


AHEAD = 2
LAG_TWO = 1
LAG_THREE = 2
LAG_FOUR = 4


def exchange_scratch(groups, nz, r, width, extra=0):
    units = groups * nz
    half = width // 2
    copies = units * 8 + 3 * groups + extra
    return [
        pltpu.VMEM((units, 4, r, width), BF16),
        pltpu.VMEM((units, 4, r, width), BF16),
        pltpu.VMEM((units, 2, r, half), BF16),
        pltpu.VMEM((units, 2, r, half), BF16),
        pltpu.VMEM((units, r, half), BF16),
        pltpu.VMEM((units, r, half), BF16),
        pltpu.VMEM((groups, nz - 1, r, width), BF16),
        pltpu.VMEM((groups, r, width), BF16),
        pltpu.VMEM((groups, 3, r, width), BF16),
        pltpu.SemaphoreType.DMA((copies,)),
        pltpu.SemaphoreType.DMA((copies,)),
        pltpu.SemaphoreType.DMA((units,)),
    ]


def backward_kernel(
    qa_ref, k_ref, v_ref, o_ref, do_ref, kbias_ref, a1_ref, of_ref, dy_ref, x_ref, dr_ref, w_ref, vec_ref,
    s_bo_ref, s_g2_ref, s_h2_ref, s_bd_ref, s_bu_ref, up_send, up_keep, down_send, down_keep,
    out_ref, up_ref, down_ref, qkv_ref, wo_ref, sums_ref,
    mask_ref, doa_ref, dqt_ref, dq_ref, dk_ref, dv_ref, a1t_ref, res_ref, late_ref, small_in, *scratch,
):
    ex = Exchange((down_send, up_send), (down_keep, up_keep), late_ref, *scratch[:9], scratch[9:])
    pid = pl.program_id(0)
    width = x_ref.shape[1]
    nz = ex.nz
    r = late_ref.shape[2]
    heads, tiles = 6, 4
    last_slot = 2 * heads + 4 + tiles

    plan = {}
    for t in range(ex.steps()):
        early = t * (2 * heads + 4) // (2 * nz)
        late = 2 * heads + 4 + (t - 2 * nz) * 8 // nz
        plan.setdefault(min(last_slot, early if t < 2 * nz else late), []).append(t)

    def at_slot(slot):
        for t in plan.get(slot, ()):
            ex.step(t)

    @pl.when(pid == 0)
    def _():
        ex.barrier()
        ex.start()
        sums_ref[...] = jnp.zeros_like(sums_ref)
        for i, ref in enumerate((s_bo_ref, s_g2_ref, s_h2_ref, s_bd_ref)):
            sums_ref[4 + i : 5 + i, :] = ref[...]
        for i in range(4):
            sums_ref[8 + i : 9 + i, :] = s_bu_ref[:, i * width : (i + 1) * width]

    def between(half):
        for step in range(heads):
            if 2 * step + half in plan:
                @pl.when(pid == step)
                def _():
                    at_slot(2 * step + half)

    @pl.when(pid < heads)
    def _():
        cols = pl.ds(pl.multiple_of(pid * 128, 128), 128)
        attn_bwd_kernel(
            qa_ref, k_ref, v_ref, o_ref, do_ref, kbias_ref, dq_ref.at[:, cols], dk_ref.at[:, cols],
            dv_ref.at[:, cols], mask_ref, doa_ref, dqt_ref, between=between,
        )

    first = ex.units - nz
    for block, right in enumerate((dq_ref, dk_ref, dv_ref, dy_ref)):
        @pl.when(pid == heads + block)
        def _():
            at_slot(2 * heads + block)
            if block == 0:
                a1t_ref[...] = a1_ref[...].T
            if block < 3:
                res_ref[...] = mm(a1t_ref[...], right[...])
            else:
                res_ref[...] = mm_tn(of_ref[...], right[...])
            for j in range(nz):
                base = ex.owner(j) * (2 * r)
                there = pl.multiple_of(base + (1 - ex.c) * r, 8)
                here = pl.multiple_of(base + ex.c * r, 8)
                late_ref[block, j] = res_ref[pl.ds(there, r), :].astype(BF16)
                ex.mine[first + j, block] = res_ref[pl.ds(here, r), :].astype(BF16)
            ex.late_copy(block).start()

    for tile in range(tiles):
        @pl.when(pid == heads + 4 + tile)
        def _():
            at_slot(2 * heads + 4 + tile)

    @pl.when(pid >= heads + 4)
    def _():
        size = x_ref.shape[0]
        here = pl.ds(pl.multiple_of((pid - heads - 4) * size, size), size)
        xhat, inv_std = norm_forward(x_ref[...].astype(F32))
        dq, dk, dv = dq_ref[here, :], dk_ref[here, :], dv_ref[here, :]
        da = mm_nt(dq, w_ref[0])
        da += mm_nt(dk, w_ref[1])
        da += mm_nt(dv, w_ref[2])
        for i, value in enumerate((da * xhat, da, dq.astype(F32), dv.astype(F32))):
            sums_ref[i : i + 1, :] += jnp.sum(value, axis=0, keepdims=True)
        out_ref[...] = dr_ref[...] + norm_backward(da, xhat, inv_std, vec_ref[0:1, :])

    @pl.when(pid == heads + 4 + tiles - 1)
    def _():
        base = ex.units * 8 + 3 * ex.groups
        hops = [(ex.d, ex.mate), (ex.x, ex.f), (ex.y, ex.f)]
        small = []

        def begin(device):
            i = len(small)
            made = ex.remote(sums_ref, small_in.at[i], base + i, device)
            made.start()
            small.append(made)

        def end():
            made = small[-1]
            made.wait()
            sums_ref[...] += small_in[len(small) - 1]

        todo = list(plan.get(last_slot, ()))
        begin(hops[0])
        for i, t in enumerate(todo):
            ex.step(t)
            if i < 3:
                end()
                if i < 2:
                    begin(hops[i + 1])
        for k in range(1, nz):
            begin((ex.d, lax.rem(ex.z + k, nz) * 2 + ex.c))
        ex.stage_four(2)
        for block, value in ex.blocks(0):
            down_ref[pl.ds(pl.multiple_of(block * r, 8), r), :] = value
        for block, value in ex.blocks(1):
            up_ref[:, pl.ds(pl.multiple_of(block * width, 128), width)] = value
        for made in small[3:]:
            made.wait()
        total_small = sums_ref[...]
        for k in range(1, nz):
            total_small = total_small + small_in[2 + k]
        sums_ref[...] = total_small
        for block, value in ex.blocks(2):
            @pl.when(block < 3)
            def _():
                qkv_ref[:, pl.ds(pl.multiple_of(block * width, 128), width)] = value

            @pl.when(block == 3)
            def _():
                wo_ref[...] = value
        ex.finish()


def backward(qa, qkv, o, do, kbias, a1, dy, x, dr, ab, vecs, smalls, up_halves, down_halves, nz):
    rows, width = o.shape
    pairs = width // 128
    r = up_halves[0].shape[2]
    tile = rows // 4

    def part(p):
        return pl.BlockSpec((rows, 128), lambda i: (0, p * pairs + jnp.minimum(i, pairs - 1)))

    def row():
        return pl.BlockSpec((tile, width), lambda i: (jnp.maximum(i - pairs - 4, 0), 0))

    def f32(*shape):
        return jax.ShapeDtypeStruct(shape, F32)

    any_spec = pl.BlockSpec(memory_space=pl.ANY)
    return pl.pallas_call(
        backward_kernel,
        grid=(pairs + 8,),
        in_specs=[
            pl.BlockSpec((rows, 256), lambda i: (0, jnp.minimum(i, pairs - 1))), part(1), part(2), part(0), part(0),
            whole(kbias.shape), whole(a1.shape), whole(o.shape), whole(dy.shape), row(), row(),
            whole((3, width, width)), whole(vecs.shape),
        ] + [whole(s.shape) for s in smalls] + [any_spec] * 4,
        out_specs=[
            row(), whole((r, 4 * width)), whole((4 * r, width)), whole((r, 3 * width)), whole((r, width)),
            whole((16, width)),
        ],
        out_shape=[
            f32(rows, width), f32(r, 4 * width), f32(4 * r, width), f32(r, 3 * width), f32(r, width), f32(16, width),
        ],
        scratch_shapes=[
            pltpu.VMEM((rows // TILE, TILE, TILE), F32),
            pltpu.VMEM((rows, 128), BF16),
            pltpu.VMEM((128, rows), F32),
            pltpu.VMEM((rows, width), BF16),
            pltpu.VMEM((rows, width), BF16),
            pltpu.VMEM((rows, width), BF16),
            pltpu.VMEM((width, rows), BF16),
            pltpu.VMEM((width, width), F32),
            pltpu.VMEM((4, nz, r, width), BF16),
            pltpu.VMEM((2 + nz, 16, width), F32),
        ] + exchange_scratch(3, nz, r, width, 2 + nz),
        compiler_params=params(collective_id=1, has_side_effects=True),
        cost_estimate=cost(20 * rows * rows * width + 14 * rows * width * width, 40 * rows * width),
        name="backward",
    )(qa, qkv, qkv, o, do, kbias, a1, o, dy, x, dr, ab, vecs, *smalls, *up_halves, *down_halves)


def per_device(
    tokens, lengths, cells, cotangent, ln1_gain, ln1_bias, w_qkv, b_query, b_value, w_out, b_out,
    ln2_gain, ln2_bias, w_up, b_up, w_down, b_down,
):
    seqs, context, width = tokens.shape
    r = w_qkv.shape[0]
    nf = width // r
    nz = nf // 2
    f = lax.axis_index("fsdp")
    ids = jnp.stack([lax.axis_index("dp"), f // 2, f % 2]).astype(jnp.int32)
    vectors = (ln1_gain, ln1_bias, b_query, b_value, b_out, ln2_gain, ln2_bias, b_down)
    small = jnp.concatenate([v[None] for v in vectors] + [b_up.reshape(4, r)])
    small = jnp.pad(small, ((0, 4), (0, 128 - r)))
    x = tokens[0]
    if r % 16 == 0:
        ab, down_full, vecs, bu, kbias, a1, qkv, o, qa = head_forward(
            w_qkv, w_out, w_up, w_down, small, x, cells, lengths, nz
        )
        ab = ab.reshape(8, width, width)
    else:
        own = jnp.stack(
            [w_qkv[:, i * width : (i + 1) * width] for i in range(3)]
            + [w_out]
            + [w_up[:, i * width : (i + 1) * width] for i in range(4)]
            + [w_down[i * r : (i + 1) * r] for i in range(4)]
        )
        ab, down_full, smalls = gather_weights(own, small, nz)
        ab = ab.reshape(8, width, width)
        smalls = smalls[:, :, :r].astype(F32)
        vecs = smalls.transpose(1, 0, 2).reshape(16, width)
        bu = smalls[:, 8:12].reshape(1, 4 * width)
        kbias, rbias = mask_terms(lengths, cells, context)
        a1, qkv = qkv_forward(x, ab, vecs, 0.125)
        o, qa = attn_forward(qkv, kbias, rbias)
    down_full = down_full.reshape(4 * width, width)
    out, dm, a2, g, du, dr, dy, do, s_g2, s_h2, s_bu, s_bd, s_bo = mlp_both(
        x, o, cotangent[0], lengths, ab, down_full, vecs, bu
    )
    down_halves = grad_down_split(ids, g, dm, nz)
    up_halves = grad_up_split(ids, a2, du, nz)
    grad_x, grad_up, grad_down, grad_qkv, grad_out, sums = backward(
        qa, qkv, o, do, kbias, a1, dy, x, dr, ab, vecs, (s_bo, s_g2, s_h2, s_bd, s_bu), up_halves, down_halves, nz
    )
    mine = lax.dynamic_slice(sums, (0, f * r), (8, r))
    g_g1, g_h1, g_bq, g_bv, g_bo, g_g2, g_h2, g_bd = (mine[i] for i in range(8))
    g_bu = lax.dynamic_slice(sums[8:12].reshape(-1), (f * 4 * r,), (4 * r,))
    return (
        out[None], grad_x[None], g_g1, g_h1, grad_qkv, g_bq, g_bv, grad_out, g_bo, g_g2, g_h2,
        grad_up, g_bu, grad_down, g_bd,
    )


def solution(mesh):
    split = P(("dp", "fsdp"), None, None)
    vec, mat = P("fsdp"), P("fsdp", None)
    in_specs = (
        split, P(("dp", "fsdp")), P(("dp", "fsdp"), None), split,
        vec, vec, mat, vec, vec, mat, vec, vec, vec, mat, vec, mat, vec,
    )
    out_specs = (split, split, vec, vec, mat, vec, vec, mat, vec, vec, vec, mat, vec, mat, vec)
    return jax.shard_map(
        per_device, mesh=mesh, in_specs=in_specs, out_specs=out_specs, check_vma=False
    )
```
